32 devices in a mesh: tm: 4 (over y, x), chan: 8 (over z, core).
Axes of the slice: x: 2, y: 2, z: 4, core: 2. Of those that a mesh axis runs over, the one named last changes fastest.
Arguments:
- samples: bfloat16 [1024, 131072], P('tm', 'chan'), may hold values from -6 to 6
- valid: int32 [1024, 16], P('tm', 'chan'), may hold values from 0 to 1, as said below
Outputs:
- average: float32 [1024, 4224], P(('tm', 'chan'))
The draws below stay inside these ranges and needn't reach their ends.
Inputs may be any that keep to these rules, and one draw needn't show every extreme that they name: `valid`: split the channels into aligned groups of 256; in every segment each group has at most 192 entries equal to 1, and exactly 192 for some group and segment; at least one channel has no 1 in any segment.
All inputs are finite; a program needn't handle non-finite values.
Results may differ from the reference program's by a relative error of at most 0.0026.
Values may be sent and summed in bfloat16 or wider, within the bound.
No kernel may reach another device: no remote copies, remote signals or barrier semaphores. Data moves between devices by JAX's collectives and lax.ppermute only.
A program may use at most 128 MiB of HBM per device.

```python
import jax
import jax.numpy as jnp
from jax import lax

CHANNELS = 1024
RADIX = 128
KBANDS = 33
SEGMENTS = 16
TIME = 131072
MOSTV = 192
N_TM = 4


def draw_samples(key, part):
    streams = jax.random.split(jax.random.fold_in(key, 17), 3)
    offset = jax.random.uniform(streams[0], (CHANNELS, 1), jnp.float32, -1.5, 1.5)
    values = offset + jax.random.normal(streams[2], (CHANNELS, TIME), jnp.float32)
    return jnp.clip(values, -6.0, 6.0).astype(jnp.bfloat16)


def draw_valid(key, part):
    keys = jax.random.split(key, 5)
    cluster_size_number = CHANNELS // N_TM
    cell_index = jnp.arange(N_TM * SEGMENTS, dtype=jnp.int32).reshape(N_TM, SEGMENTS)
    channel_index = jnp.arange(CHANNELS, dtype=jnp.int32)
    per_cell = jax.random.randint(keys[0], (N_TM, SEGMENTS), cluster_size_number // 8, MOSTV + 1)
    fullest = jax.random.randint(keys[1], (), 0, N_TM * SEGMENTS)
    per_cell = jnp.where(cell_index == fullest, MOSTV, per_cell)
    missing_jitter_term = jax.random.randint(keys[2], (CHANNELS,), 0, 32) == 0
    dead_forced = channel_index == jax.random.randint(keys[3], (), 0, CHANNELS)
    priority_levels = jax.random.randint(keys[4], (N_TM, SEGMENTS, cluster_size_number), 0, 1 << 16)
    missing_reward = jnp.where(missing_jitter_term, 1 << 16, 0).reshape(N_TM, 1, cluster_size_number)
    priority_levels = priority_levels + missing_reward
    priority_levels = jnp.where(dead_forced.reshape(N_TM, 1, cluster_size_number), 1 << 17, priority_levels)
    inside = jnp.arange(cluster_size_number, dtype=jnp.int32)
    distinct = priority_levels * cluster_size_number + inside[None, None, :]
    order = jnp.argsort(distinct, axis=2)
    ranking = jnp.argsort(order, axis=2)
    chosen = (ranking < per_cell[:, :, None]).astype(jnp.int32)
    return jnp.transpose(chosen, (0, 2, 1)).reshape(CHANNELS, SEGMENTS)


def setup_inputs(seed: int = 0) -> dict:
    arg_keys = jax.random.split(jax.random.key(seed), 3)
    samples = draw_samples(jax.random.fold_in(arg_keys[2], 71), 0)
    valid = draw_valid(jax.random.fold_in(arg_keys[2], 71), 0)
    return {"samples": samples, "valid": valid}


full_turn = 6.283185307179586


def make_tables():
    seg_len = RADIX * RADIX
    counter = jnp.arange(RADIX, dtype=jnp.int32)
    inner_prod = (counter[:, None] * counter[None, :]) % RADIX
    angle_one = full_turn * inner_prod.astype(jnp.float32) / RADIX
    cos_one = jnp.cos(angle_one).astype(jnp.bfloat16)
    sin_one = jnp.sin(angle_one).astype(jnp.bfloat16)
    outer_prod = (counter[:, None] * counter[None, :]) % seg_len
    angle_mid = full_turn * outer_prod.astype(jnp.float32) / seg_len
    twid_real = jnp.cos(angle_mid)
    twid_imag = -jnp.sin(angle_mid)
    band_index = jnp.arange(KBANDS, dtype=jnp.int32)
    angle_two = full_turn * ((counter[:, None] * band_index[None, :]) % RADIX).astype(jnp.float32) / RADIX
    cos_two = jnp.cos(angle_two).astype(jnp.bfloat16)
    sine_double_angle = jnp.sin(angle_two).astype(jnp.bfloat16)
    places = jnp.arange(seg_len, dtype=jnp.int32).astype(jnp.float32)
    window = 0.5 - 0.5 * jnp.cos(full_turn * places / seg_len)
    weight_sum = jnp.sum(window * window)
    onesided = jnp.where(jnp.arange(KBANDS * RADIX, dtype=jnp.int32) == 0, 1.0, 2.0).astype(jnp.float32) / weight_sum
    return (cos_one, sin_one, twid_real, twid_imag, cos_two, sine_double_angle, window, onesided)


def contract(left, right, form):
    return jnp.einsum(form, left.astype(jnp.float32), right.astype(jnp.float32))


def spectrum(segment, tables):
    cos_one, sin_one, twid_real, twid_imag, cos_two, sine_double_angle, window, onesided = tables
    height = segment.shape[0]
    values = segment.astype(jnp.float32)
    centred = values - jnp.mean(values, axis=1, keepdims=True)
    shaped = (centred * window[None, :]).astype(jnp.bfloat16).reshape(height, RADIX, RADIX)
    first_real = contract(shaped, cos_one, "cnm,nk->ckm")
    first_imag = -contract(shaped, sin_one, "cnm,nk->ckm")
    mid_real = (first_real * twid_real - first_imag * twid_imag).astype(jnp.bfloat16)
    mid_imag = (first_real * twid_imag + first_imag * twid_real).astype(jnp.bfloat16)
    last_real = contract(mid_real, cos_two, "ckn,nm->cmk") + contract(mid_imag, sine_double_angle, "ckn,nm->cmk")
    closing_quadrature_part = contract(mid_imag, cos_two, "ckn,nm->cmk") - contract(mid_real, sine_double_angle, "ckn,nm->cmk")
    return (last_real * last_real + closing_quadrature_part * closing_quadrature_part).reshape(height, -1) * onesided[None, :]


def block_power(segments, tables):
    height = segments.shape[0]
    block_rows = 128 if height % 128 == 0 else height

    def one_block(piece):
        return spectrum(piece, tables)

    final_output = lax.map(one_block, segments.reshape(height // block_rows, block_rows, -1))
    return final_output.reshape(height, -1)


def reference(samples, valid):
    tables = make_tables()
    seg_len = RADIX * RADIX
    half_len = seg_len // 2
    padded = jnp.concatenate([samples, jnp.zeros((CHANNELS, half_len), jnp.bfloat16)], axis=1)

    def accumulate(cumulative_tally, segment_index):
        start = (segment_index * half_len).astype(jnp.int32)
        segment = lax.dynamic_slice_in_dim(padded, start, seg_len, 1)
        powers = block_power(segment, tables)
        weights = lax.dynamic_slice_in_dim(valid, segment_index, 1, 1).astype(jnp.float32)
        return cumulative_tally + weights * powers, None

    initial = jnp.zeros((CHANNELS, KBANDS * RADIX), jnp.float32)
    totals, _ = lax.scan(accumulate, initial, jnp.arange(SEGMENTS, dtype=jnp.int32))
    tallied_count = jnp.sum(valid, axis=1).astype(jnp.float32)
    return totals / jnp.maximum(tallied_count, 1.0)[:, None]
```

```python
import functools

import jax
import jax.numpy as jnp
import numpy as np
from jax import lax
from jax.experimental import pallas as pl
from jax.experimental.pallas import tpu as pltpu
from jax.sharding import PartitionSpec as P

RADIX = 128
KBANDS = 33
SUB = 8
PAD = 40
HALF = RADIX // 2
ROWS = SUB * KBANDS + SUB
SEG = RADIX * RADIX


def make_tables():
    counter = np.arange(RADIX)
    angle = 2 * np.pi * ((counter[:, None] * counter[None, :]) % RADIX) / RADIX
    first = np.concatenate([np.cos(angle), -np.sin(angle)], axis=1)
    mid = 2 * np.pi * (counter[:, None] * counter[None, :]) / SEG
    twiddle = np.stack([np.cos(mid), -np.sin(mid)])
    second = np.zeros((2 * PAD, 2 * RADIX))
    cos2, sin2 = np.cos(angle[:KBANDS]), np.sin(angle[:KBANDS])
    second[:KBANDS, :RADIX], second[:KBANDS, RADIX:] = cos2, sin2
    second[PAD : PAD + KBANDS, :RADIX], second[PAD : PAD + KBANDS, RADIX:] = -sin2, cos2
    window = (0.5 - 0.5 * np.cos(2 * np.pi * np.arange(SEG) / SEG)).astype(np.float32)
    scale = np.full((KBANDS, RADIX), 2.0)
    scale[0, 0] = 1.0
    scale = scale / np.sum(window.astype(np.float64) ** 2)
    return (
        jnp.asarray(first, jnp.bfloat16),
        jnp.asarray(twiddle, jnp.float32),
        jnp.asarray(second, jnp.bfloat16),
        jnp.asarray(window.reshape(RADIX, RADIX)),
        jnp.asarray(scale, jnp.float32),
    )


def stage(dst, sums, source):
    value = source.astype(jnp.float32)
    dst[...] = value.reshape(HALF * SUB, RADIX)
    total = jnp.sum(jnp.sum(value, axis=0), axis=1, keepdims=True)
    sums[...] = jnp.broadcast_to(total, (SUB, RADIX))


def segment_power(c, head, tail, head_sum, tail_sum, tables):
    first_ref, twiddle_ref, second_ref, window_ref = tables
    value = jnp.concatenate(
        [head[pl.ds(c, HALF, stride=SUB), :], tail[pl.ds(c, HALF, stride=SUB), :]], axis=0
    )
    mean = (head_sum[c : c + 1, :] + tail_sum[c : c + 1, :]) * (1.0 / SEG)
    shaped = ((value - mean) * window_ref[...]).astype(jnp.bfloat16)
    first = jnp.dot(shaped.T, first_ref[...], preferred_element_type=jnp.float32)
    real, imag = first[:, :RADIX], first[:, RADIX:]
    turn_real, turn_imag = twiddle_ref[0], twiddle_ref[1]
    middle = jnp.concatenate(
        [
            (real * turn_real - imag * turn_imag).astype(jnp.bfloat16),
            (real * turn_imag + imag * turn_real).astype(jnp.bfloat16),
        ],
        axis=0,
    )
    spectrum = jnp.dot(second_ref[...], middle, preferred_element_type=jnp.float32)
    real, imag = spectrum[:PAD], spectrum[PAD:]
    return real * real + imag * imag


def local_kernel(where, own, other, weight, first, twiddle, second, window, out, wide, sums):
    core = where[0]
    for half in range(2):
        rows = slice(half * HALF, (half + 1) * HALF)
        stage(wide.at[core, half], sums.at[core, half], own[0, rows])
        stage(wide.at[1 - core, half], sums.at[1 - core, half], other[0, rows])
    tables = (first, twiddle, second, window)
    pieces = ((0, 0, 0, 1), (0, 1, 1, 0), (1, 0, 1, 1))
    for c in range(SUB):
        total = None
        for s, (b0, h0, b1, h1) in enumerate(pieces):
            power = segment_power(
                c, wide.at[b0, h0], wide.at[b1, h1], sums.at[b0, h0], sums.at[b1, h1], tables
            )
            power = power * weight[0, s, c : c + 1, :]
            total = power if total is None else total + power
        out[0, c] = total


def cross_kernel(
    groups, where, own, other, lower0, lower1, upper0, upper1, base, weight,
    first, twiddle, second, window, out, wide, sums, total,
):
    core, chip, parity = where[0], where[1], where[2]
    group = 2 * pl.program_id(0) + parity
    low = group < groups // 2
    tables = (first, twiddle, second, window)
    total[...] = base[0]

    def put(slot, first_source, second_source, pick, half):
        rows = slice(half * HALF, (half + 1) * HALF)

        @pl.when(pick)
        def _():
            stage(wide.at[slot], sums.at[slot], first_source[0, rows])

        @pl.when(jnp.logical_not(pick))
        def _():
            stage(wide.at[slot], sums.at[slot], second_source[0, rows])

    def add(s):
        for c in range(SUB):
            power = segment_power(c, wide.at[0], wide.at[1], sums.at[0], sums.at[1], tables)
            total[c] = total[c] + power * weight[0, s, c : c + 1, :]

    @pl.when(jnp.logical_or(low, chip == groups - 1))
    def _():
        put(0, own, other, core == 1, 1)

        @pl.when(low)
        def _():
            put(1, upper0, upper1, core == 0, 0)

        @pl.when(jnp.logical_not(low))
        def _():
            wide[1] = jnp.zeros_like(wide[1])
            sums[1] = jnp.zeros_like(sums[1])

        add(3)

    @pl.when(jnp.logical_and(jnp.logical_not(low), chip > 0))
    def _():
        put(0, lower0, lower1, core == 0, 0)
        put(1, own, other, core == 0, 0)
        add(4)

    count = jnp.sum(weight[0, :4], axis=0)
    packed = jnp.concatenate([total[c, :KBANDS] for c in range(SUB)] + [count], axis=0)
    out[0, 0] = packed.astype(out.dtype)


def finish_kernel(keep, got, scale, out, total):
    total[...] = keep[0] + got[0].astype(jnp.float32)
    count = jnp.maximum(total[SUB * KBANDS :, :], 1.0)
    inverse = 1.0 / count
    for j in range(KBANDS):
        value = total[pl.ds(j, SUB, stride=KBANDS), :]
        out[:, j * RADIX : (j + 1) * RADIX] = value * scale[j : j + 1, :] * inverse


def whole(array):
    return pl.BlockSpec(array.shape, lambda *_: (0,) * array.ndim)


def per_device(samples, valid):
    first, twiddle, second, window, scale = make_tables()
    tables = (first, twiddle, second, window)
    channels = samples.shape[0]
    size = lax.axis_size("chan")
    chips = size // 2
    place = lax.axis_index("chan")
    core, chip = place % 2, place // 2
    sub = channels // (SUB * size)
    tiles = samples.reshape(channels // SUB, SUB, RADIX, RADIX).transpose(0, 2, 1, 3)
    groups = tiles.reshape(chips, 2, sub, RADIX, SUB, RADIX)
    half = chips // 2

    def send(value, perm):
        return lax.ppermute(value, "chan", perm)

    swap = [(i, i ^ 1) for i in range(size)]
    links = range(chips - 1)
    lower = [
        send(groups[half:, c, :, HALF:], [(2 * z + 1, 2 * z + 2 + c) for z in links])
        for c in range(2)
    ]
    upper = [
        send(groups[:half, c, :, :HALF], [(2 * z + 2, 2 * z + c) for z in links])
        for c in range(2)
    ]
    lower = [v.reshape(half * sub, HALF, SUB, RADIX) for v in lower]
    upper = [v.reshape(half * sub, HALF, SUB, RADIX) for v in upper]
    other = send(lax.dynamic_index_in_dim(groups, 1 - core, 1, False), swap)
    other = other.reshape(chips * sub, RADIX, SUB, RADIX)

    theirs = send(valid, swap)
    both = jnp.where(core == 0, jnp.concatenate([valid, theirs], 1), jnp.concatenate([theirs, valid], 1))
    before = send(both, [(i, i + 2) for i in range(size - 2)])
    weight = jnp.concatenate([both, before[:, 3:]], axis=1).astype(jnp.float32)
    weight = weight.reshape(chips, 2, sub, SUB, 5)
    weight = lax.dynamic_index_in_dim(weight, core, 1, False).reshape(chips * sub, SUB, 5)
    weight = jnp.broadcast_to(weight.transpose(0, 2, 1)[..., None], (chips * sub, 5, SUB, RADIX))

    tile = (1, RADIX, SUB, RADIX)
    part = (1, HALF, SUB, RADIX)
    wide_shape = pltpu.VMEM((2, 2, HALF * SUB, RADIX), jnp.float32)
    sums_shape = pltpu.VMEM((2, 2, SUB, RADIX), jnp.float32)
    partial = pl.pallas_call(
        local_kernel,
        grid_spec=pltpu.PrefetchScalarGridSpec(
            num_scalar_prefetch=1,
            grid=(chips, sub),
            in_specs=[
                pl.BlockSpec(tile, lambda g, i, w: ((2 * g + w[0]) * sub + i, 0, 0, 0)),
                pl.BlockSpec(tile, lambda g, i, w: (g * sub + i, 0, 0, 0)),
                pl.BlockSpec((1, 5, SUB, RADIX), lambda g, i, w: (g * sub + i, 0, 0, 0)),
                *[whole(t) for t in tables],
            ],
            out_specs=pl.BlockSpec((1, SUB, PAD, RADIX), lambda g, i, w: (g * sub + i, 0, 0, 0)),
            scratch_shapes=[wide_shape, sums_shape],
        ),
        out_shape=jax.ShapeDtypeStruct((chips * sub, SUB, PAD, RADIX), jnp.float32),
        name="local_segments",
    )(core[None].astype(jnp.int32), tiles, other, weight, *tables)

    def cross(parity, dtype, name):
        def mine(g, i, w):
            return ((2 * (2 * g + w[2]) + w[0]) * sub + i, 0, 0, 0)

        def dense(g, i, w):
            return ((2 * g + w[2]) * sub + i, 0, 0, 0)

        def low(g, i, w):
            return (jnp.minimum(2 * g + w[2], half - 1) * sub + i, 0, 0, 0)

        def high(g, i, w):
            return (jnp.maximum(2 * g + w[2] - half, 0) * sub + i, 0, 0, 0)

        where = jnp.stack([core, chip, parity]).astype(jnp.int32)
        return pl.pallas_call(
            functools.partial(unpack_where, chips),
            grid_spec=pltpu.PrefetchScalarGridSpec(
                num_scalar_prefetch=1,
                grid=(half, sub),
                in_specs=[
                    pl.BlockSpec(tile, mine),
                    pl.BlockSpec(tile, dense),
                    pl.BlockSpec(part, high),
                    pl.BlockSpec(part, high),
                    pl.BlockSpec(part, low),
                    pl.BlockSpec(part, low),
                    pl.BlockSpec((1, SUB, PAD, RADIX), dense),
                    pl.BlockSpec((1, 5, SUB, RADIX), dense),
                    *[whole(t) for t in tables],
                ],
                out_specs=pl.BlockSpec((1, 1, ROWS, RADIX), lambda g, i, w: (g, i, 0, 0)),
                scratch_shapes=[
                    pltpu.VMEM((2, HALF * SUB, RADIX), jnp.float32),
                    pltpu.VMEM((2, SUB, RADIX), jnp.float32),
                    pltpu.VMEM((SUB, PAD, RADIX), jnp.float32),
                ],
            ),
            out_shape=jax.ShapeDtypeStruct((half, sub, ROWS, RADIX), dtype),
            name=name,
        )(where, tiles, other, *lower, *upper, partial, weight, *tables)

    bit = chip % 2
    away = cross(1 - bit, jnp.bfloat16, "cross_away")
    got = send(away, [(i, i ^ 2) for i in range(size)])
    keep = cross(bit, jnp.float32, "cross_keep")
    step = 4
    while keep.shape[0] > 1:
        keep = keep + got.astype(jnp.float32)
        pairs = keep.reshape(keep.shape[0] // 2, 2, *keep.shape[1:])
        bit = (place // step) % 2
        away = lax.dynamic_index_in_dim(pairs, 1 - bit, 1, False).astype(jnp.bfloat16)
        got = send(away, [(i, i ^ step) for i in range(size)])
        keep = lax.dynamic_index_in_dim(pairs, bit, 1, False)
        step *= 2

    return pl.pallas_call(
        finish_kernel,
        grid=(sub,),
        in_specs=[
            pl.BlockSpec((1, ROWS, RADIX), lambda i: (i, 0, 0)),
            pl.BlockSpec((1, ROWS, RADIX), lambda i: (i, 0, 0)),
            whole(scale),
        ],
        out_specs=pl.BlockSpec((SUB, KBANDS * RADIX), lambda i: (i, 0)),
        out_shape=jax.ShapeDtypeStruct((sub * SUB, KBANDS * RADIX), jnp.float32),
        scratch_shapes=[pltpu.VMEM((ROWS, RADIX), jnp.float32)],
        name="finish",
    )(keep[0], got[0], scale)


def unpack_where(chips, where, *refs):
    cross_kernel(chips, where, *refs)


def solution(mesh):
    return jax.shard_map(
        per_device,
        mesh=mesh,
        in_specs=(P("tm", "chan"), P("tm", "chan")),
        out_specs=P(("tm", "chan"), None),
        check_vma=False,
    )
```

```python
import functools

import jax
import jax.numpy as jnp
import numpy as np
from jax import lax
from jax.experimental import pallas as pl
from jax.experimental.pallas import tpu as pltpu
from jax.sharding import PartitionSpec as P

RADIX = 128
KBANDS = 33
SUB = 8
HALF = RADIX // 2
STEP = HALF + 4
OUT = 72
ROWS = SUB * KBANDS + SUB
SEG = RADIX * RADIX
SLOTS = 6


def make_tables():
    counter = np.arange(RADIX)
    angle = 2 * np.pi * ((counter[:, None] * counter[None, :]) % RADIX) / RADIX
    cos, sin = np.cos(angle), np.sin(angle)
    first = np.block([[cos, -sin], [sin, cos]])
    mid = 2 * np.pi * (counter[:, None] * counter[None, :]) / SEG
    twiddle = np.stack([np.cos(mid), -np.sin(mid)])
    bands = np.concatenate([np.arange(KBANDS), RADIX - np.arange(KBANDS + 1)]) % RADIX
    second = np.zeros((2 * OUT, 2 * RADIX))
    size = len(bands)
    second[:size, :RADIX], second[:size, RADIX:] = cos[bands], sin[bands]
    second[OUT : OUT + size, :RADIX], second[OUT : OUT + size, RADIX:] = -sin[bands], cos[bands]
    window = (0.5 - 0.5 * np.cos(2 * np.pi * np.arange(SEG) / SEG)).astype(np.float32)
    mirror = np.zeros((RADIX, RADIX))
    mirror[(RADIX - counter) % RADIX, counter] = 1.0
    scale = np.full((KBANDS, RADIX), 2.0)
    scale[0, 0] = 1.0
    scale = 0.5 * scale / np.sum(window.astype(np.float64) ** 2)
    return (
        jnp.asarray(first, jnp.bfloat16),
        jnp.asarray(twiddle, jnp.float32),
        jnp.asarray(second, jnp.bfloat16),
        jnp.asarray(window.reshape(RADIX, RADIX)),
        jnp.asarray(mirror, jnp.bfloat16),
        jnp.asarray(scale, jnp.float32),
    )


def stage(dst, sums, source, half):
    total = [None] * 4
    for a in range(HALF):
        value = source[0, half * HALF + a].astype(jnp.float32)
        dst[pl.ds(a, SUB, stride=STEP), :] = value
        total[a % 4] = value if total[a % 4] is None else total[a % 4] + value
    total = (total[0] + total[1]) + (total[2] + total[3])
    sums[...] = jnp.broadcast_to(jnp.sum(total, axis=1, keepdims=True), (SUB, RADIX))


def pair_power(pieces, tables, lhs, mids, put):
    first_ref, twiddle_ref, second_ref, window_ref = tables
    for c in range(SUB):
        for s, (head, tail, head_sum, tail_sum, mask) in enumerate(pieces):
            rows = slice(c * STEP, c * STEP + HALF)
            value = jnp.concatenate([head[rows, :], tail[rows, :]], axis=0)
            mean = (head_sum[c : c + 1, :] + tail_sum[c : c + 1, :]) * (1.0 / SEG)
            shaped = ((value - mean) * window_ref[...]).astype(jnp.bfloat16)
            shaped = shaped * mask[c : c + 1, :].astype(jnp.bfloat16)
            lhs[c, :, s * RADIX : (s + 1) * RADIX] = shaped.T
    for c in range(SUB):
        first = jnp.dot(lhs[c], first_ref[...], preferred_element_type=jnp.float32)
        real, imag = first[:, :RADIX], first[:, RADIX:]
        turn_real, turn_imag = twiddle_ref[0], twiddle_ref[1]
        lanes = slice((c % 2) * RADIX, (c % 2 + 1) * RADIX)
        mids[c // 2, :RADIX, lanes] = (real * turn_real - imag * turn_imag).astype(jnp.bfloat16)
        mids[c // 2, RADIX:, lanes] = (real * turn_imag + imag * turn_real).astype(jnp.bfloat16)
    for i in range(SUB // 2):
        spectrum = jnp.dot(second_ref[...], mids[i], preferred_element_type=jnp.float32)
        real, imag = spectrum[:OUT], spectrum[OUT:]
        power = real * real + imag * imag
        put(2 * i, power[:, :RADIX])
        put(2 * i + 1, power[:, RADIX:])


def local_kernel(
    where, own, other, weight, first, twiddle, second, window, out, wide, sums, lhs, mids
):
    core = where[0]
    for half in range(2):
        stage(wide.at[core, half], sums.at[core, half], own, half)
        stage(wide.at[1 - core, half], sums.at[1 - core, half], other, half)
    pieces = [
        (wide.at[b, 0], wide.at[b, 1], sums.at[b, 0], sums.at[b, 1], weight.at[0, 2 * b])
        for b in range(2)
    ]

    def put(c, power):
        out[0, c] = power

    pair_power(pieces, (first, twiddle, second, window), lhs, mids, put)


def cross_kernel(
    groups, where, own, other, lower0, lower1, upper0, upper1, base, weight,
    first, twiddle, second, window, mirror, out, wide, sums, lhs, mids, total, plain, turned,
):
    core, chip, parity = where[0], where[1], where[2]
    low = 2 * pl.program_id(0) + parity < groups // 2
    high = jnp.logical_not(low)
    first_core, second_core = core == 0, core == 1
    total[...] = base[0]

    def put(slot, source, half, pick):
        @pl.when(pick)
        def _():
            stage(wide.at[slot], sums.at[slot], source, half)

    def add(c, power):
        total[c] = total[c] + power

    def one_round(r, _):
        start = r == 0
        again = r == 1

        put(0, own, 1, jnp.logical_and(start, first_core))
        put(0, other, 1, jnp.logical_and(start, second_core))
        put(1, own, 0, jnp.logical_and(start, second_core))
        put(1, other, 0, jnp.logical_and(start, first_core))
        tail = jnp.logical_and(start, low)
        put(2, own, 1, jnp.logical_and(tail, second_core))
        put(2, other, 1, jnp.logical_and(tail, first_core))
        put(3, upper0, 0, jnp.logical_and(tail, first_core))
        put(3, upper1, 0, jnp.logical_and(tail, second_core))
        tail = jnp.logical_and(start, high)
        put(2, lower0, 0, jnp.logical_and(tail, first_core))
        put(2, lower1, 0, jnp.logical_and(tail, second_core))
        put(3, own, 0, jnp.logical_and(tail, first_core))
        put(3, other, 0, jnp.logical_and(tail, second_core))
        put(0, own, 1, jnp.logical_and(again, second_core))
        put(0, other, 1, jnp.logical_and(again, first_core))

        @pl.when(again)
        def _():
            wide[1] = jnp.zeros_like(wide[1])
            sums[1] = jnp.zeros_like(sums[1])

        mask0 = jnp.where(start, 1, 3)
        mask1 = jnp.where(again, 5, jnp.where(low, 3, 4))
        pieces = [
            (wide.at[0], wide.at[1], sums.at[0], sums.at[1], weight.at[0, mask0]),
            (wide.at[2], wide.at[3], sums.at[2], sums.at[3], weight.at[0, mask1]),
        ]
        pair_power(pieces, (first, twiddle, second, window), lhs, mids, add)
        return 0

    last = jnp.logical_and(high, chip == groups - 1)
    lax.fori_loop(0, jnp.where(last, 2, 1), one_round, 0)

    lane = lax.broadcasted_iota(jnp.int32, (KBANDS, RADIX), 1)
    for c in range(SUB):
        rows = slice(c * KBANDS, (c + 1) * KBANDS)
        plain[rows, :] = total[c, :KBANDS]
        turned[rows, :] = jnp.where(
            lane == 0, total[c, KBANDS : 2 * KBANDS], total[c, KBANDS + 1 : 2 * KBANDS + 1]
        )
    plain[SUB * KBANDS :, :] = jnp.sum(weight[0, :4], axis=0)
    turned[SUB * KBANDS :, :] = jnp.zeros((SUB, RADIX), jnp.float32)
    reverse = jnp.dot(
        turned[...].astype(jnp.bfloat16), mirror[...], preferred_element_type=jnp.float32
    )
    out[0, 0] = (plain[...] + reverse).astype(out.dtype)


def finish_kernel(keep, got, scale, out, total):
    total[...] = keep[0] + got[0].astype(jnp.float32)
    count = jnp.maximum(total[SUB * KBANDS :, :], 1.0)
    inverse = 1.0 / count
    for j in range(KBANDS):
        value = total[pl.ds(j, SUB, stride=KBANDS), :]
        out[:, j * RADIX : (j + 1) * RADIX] = value * scale[j : j + 1, :] * inverse


def whole(array):
    return pl.BlockSpec(array.shape, lambda *_: (0,) * array.ndim)


def per_device(samples, valid):
    first, twiddle, second, window, mirror, scale = make_tables()
    tables = (first, twiddle, second, window)
    channels = samples.shape[0]
    size = lax.axis_size("chan")
    chips = size // 2
    half = chips // 2
    place = lax.axis_index("chan")
    core, chip = place & 1, place >> 1
    sub = channels // (SUB * size)

    def send(value, perm):
        return lax.ppermute(value, "chan", perm)

    def tiled(value):
        return value.reshape(channels // SUB, SUB, RADIX, RADIX).transpose(0, 2, 1, 3)

    swap = [(i, i ^ 1) for i in range(size)]
    links = range(chips - 1)
    tiles = tiled(samples)
    groups = tiles.reshape(chips, 2, sub, RADIX, SUB, RADIX)
    edges = [
        lax.dynamic_slice(
            groups,
            (core * half, c, 0, core * HALF, 0, 0),
            (half, 1, sub, HALF, SUB, RADIX),
        ).reshape(half * sub, HALF, SUB, RADIX)
        for c in range(2)
    ]
    lower = [send(edges[c], [(2 * z + 1, 2 * z + 2 + c) for z in links]) for c in range(2)]
    upper = [send(edges[c], [(2 * z + 2, 2 * z + c) for z in links]) for c in range(2)]
    other = tiled(send(samples, swap))

    theirs = send(valid, swap)
    before = sum(send(valid, [(2 * z + 1, 2 * z + 2 + c) for z in links]) for c in range(2))
    low = jnp.where(core == 0, valid, theirs)
    high = jnp.where(core == 0, theirs, valid)
    weight = jnp.concatenate([low, high, before[:, 1:], jnp.zeros_like(before[:, 1:])], axis=1)
    weight = weight.astype(jnp.float32).reshape(chips, 2, sub, SUB, SLOTS)
    weight = lax.dynamic_index_in_dim(weight, core, 1, False).reshape(chips * sub, SUB, SLOTS)
    weight = jnp.broadcast_to(weight.transpose(0, 2, 1)[..., None], (chips * sub, SLOTS, SUB, RADIX))

    tile = (1, RADIX, SUB, RADIX)
    part = (1, HALF, SUB, RADIX)
    stripe = STEP * SUB
    lhs_shape = pltpu.VMEM((SUB, RADIX, 2 * RADIX), jnp.bfloat16)
    mids_shape = pltpu.VMEM((SUB // 2, 2 * RADIX, 2 * RADIX), jnp.bfloat16)
    partial = pl.pallas_call(
        local_kernel,
        grid_spec=pltpu.PrefetchScalarGridSpec(
            num_scalar_prefetch=1,
            grid=(chips, sub),
            in_specs=[
                pl.BlockSpec(tile, lambda g, i, w: ((2 * g + w[0]) * sub + i, 0, 0, 0)),
                pl.BlockSpec(tile, lambda g, i, w: ((2 * g + w[0]) * sub + i, 0, 0, 0)),
                pl.BlockSpec((1, SLOTS, SUB, RADIX), lambda g, i, w: (g * sub + i, 0, 0, 0)),
                *[whole(t) for t in tables],
            ],
            out_specs=pl.BlockSpec((1, SUB, OUT, RADIX), lambda g, i, w: (g * sub + i, 0, 0, 0)),
            scratch_shapes=[
                pltpu.VMEM((2, 2, stripe, RADIX), jnp.float32),
                pltpu.VMEM((2, 2, SUB, RADIX), jnp.float32),
                lhs_shape,
                mids_shape,
            ],
        ),
        out_shape=jax.ShapeDtypeStruct((chips * sub, SUB, OUT, RADIX), jnp.float32),
        name="local_segments",
    )(core[None].astype(jnp.int32), tiles, other, weight, *tables)

    def cross(parity, dtype, name):
        def mine(g, i, w):
            return ((2 * (2 * g + w[2]) + w[0]) * sub + i, 0, 0, 0)

        def dense(g, i, w):
            return ((2 * g + w[2]) * sub + i, 0, 0, 0)

        def low(g, i, w):
            return (jnp.minimum(2 * g + w[2], half - 1) * sub + i, 0, 0, 0)

        def high(g, i, w):
            return (jnp.maximum(2 * g + w[2] - half, 0) * sub + i, 0, 0, 0)

        where = jnp.stack([core, chip, parity]).astype(jnp.int32)
        return pl.pallas_call(
            functools.partial(cross_kernel, chips),
            grid_spec=pltpu.PrefetchScalarGridSpec(
                num_scalar_prefetch=1,
                grid=(half, sub),
                in_specs=[
                    pl.BlockSpec(tile, mine),
                    pl.BlockSpec(tile, mine),
                    pl.BlockSpec(part, high),
                    pl.BlockSpec(part, high),
                    pl.BlockSpec(part, low),
                    pl.BlockSpec(part, low),
                    pl.BlockSpec((1, SUB, OUT, RADIX), dense),
                    pl.BlockSpec((1, SLOTS, SUB, RADIX), dense),
                    *[whole(t) for t in tables],
                    whole(mirror),
                ],
                out_specs=pl.BlockSpec((1, 1, ROWS, RADIX), lambda g, i, w: (g, i, 0, 0)),
                scratch_shapes=[
                    pltpu.VMEM((4, stripe, RADIX), jnp.float32),
                    pltpu.VMEM((4, SUB, RADIX), jnp.float32),
                    lhs_shape,
                    mids_shape,
                    pltpu.VMEM((SUB, OUT, RADIX), jnp.float32),
                    pltpu.VMEM((ROWS, RADIX), jnp.float32),
                    pltpu.VMEM((ROWS, RADIX), jnp.float32),
                ],
            ),
            out_shape=jax.ShapeDtypeStruct((half, sub, ROWS, RADIX), dtype),
            name=name,
        )(where, tiles, other, *lower, *upper, partial, weight, *tables, mirror)

    bit = chip & 1
    away = cross(1 - bit, jnp.bfloat16, "cross_away")
    got = send(away, [(i, i ^ 2) for i in range(size)])
    keep = cross(bit, jnp.float32, "cross_keep")
    step = 4
    while keep.shape[0] > 1:
        keep = keep + got.astype(jnp.float32)
        pairs = keep.reshape(keep.shape[0] // 2, 2, *keep.shape[1:])
        bit = (place // step) & 1
        away = lax.dynamic_index_in_dim(pairs, 1 - bit, 1, False).astype(jnp.bfloat16)
        got = send(away, [(i, i ^ step) for i in range(size)])
        keep = lax.dynamic_index_in_dim(pairs, bit, 1, False)
        step *= 2

    return pl.pallas_call(
        finish_kernel,
        grid=(sub,),
        in_specs=[
            pl.BlockSpec((1, ROWS, RADIX), lambda i: (i, 0, 0)),
            pl.BlockSpec((1, ROWS, RADIX), lambda i: (i, 0, 0)),
            whole(scale),
        ],
        out_specs=pl.BlockSpec((SUB, KBANDS * RADIX), lambda i: (i, 0)),
        out_shape=jax.ShapeDtypeStruct((sub * SUB, KBANDS * RADIX), jnp.float32),
        scratch_shapes=[pltpu.VMEM((ROWS, RADIX), jnp.float32)],
        name="finish",
    )(keep[0], got[0], scale)


def solution(mesh):
    return jax.shard_map(
        per_device,
        mesh=mesh,
        in_specs=(P("tm", "chan"), P("tm", "chan")),
        out_specs=P(("tm", "chan"), None),
        check_vma=False,
    )
```

```python
import functools

import jax
import jax.numpy as jnp
import numpy as np
from jax import lax
from jax.experimental import pallas as pl
from jax.experimental.pallas import tpu as pltpu
from jax.sharding import PartitionSpec as P


RADIX = 128
KBANDS = 33
SUB = 8
HALF = RADIX // 2
STEP = HALF + 4
OUT = 72
ROWS = SUB * KBANDS + SUB
SEG = RADIX * RADIX
SLOTS = 6


def make_tables():
    counter = np.arange(RADIX)
    angle = 2 * np.pi * ((counter[:, None] * counter[None, :]) % RADIX) / RADIX
    cos, sin = np.cos(angle), np.sin(angle)
    first = np.block([[cos, -sin], [sin, cos]])
    mid = 2 * np.pi * (counter[:, None] * counter[None, :]) / SEG
    twiddle = np.stack([np.cos(mid), -np.sin(mid)])
    bands = np.concatenate([np.arange(KBANDS), RADIX - np.arange(KBANDS + 1)]) % RADIX
    second = np.zeros((2 * OUT, 2 * RADIX))
    size = len(bands)
    second[:size, :RADIX], second[:size, RADIX:] = cos[bands], sin[bands]
    second[OUT : OUT + size, :RADIX], second[OUT : OUT + size, RADIX:] = -sin[bands], cos[bands]
    window = (0.5 - 0.5 * np.cos(2 * np.pi * np.arange(SEG) / SEG)).astype(np.float32)
    mirror = np.zeros((RADIX, RADIX))
    mirror[(RADIX - counter) % RADIX, counter] = 1.0
    scale = np.full((KBANDS, RADIX), 2.0)
    scale[0, 0] = 1.0
    scale = 0.5 * scale / np.sum(window.astype(np.float64) ** 2)
    return (
        jnp.asarray(first, jnp.bfloat16),
        jnp.asarray(twiddle, jnp.float32),
        jnp.asarray(second, jnp.bfloat16),
        jnp.asarray(window.reshape(RADIX, RADIX)),
        jnp.asarray(mirror, jnp.bfloat16),
        jnp.asarray(scale, jnp.float32),
    )


def stage(dst, sums, source, half):
    total = [None] * 4
    for a in range(HALF):
        value = source[half * HALF + a].astype(jnp.float32)
        dst[pl.ds(a, SUB, stride=STEP), :] = value
        total[a % 4] = value if total[a % 4] is None else total[a % 4] + value
    total = (total[0] + total[1]) + (total[2] + total[3])
    sums[...] = jnp.broadcast_to(jnp.sum(total, axis=1, keepdims=True), (SUB, RADIX))


def shape(c, piece, window_ref):
    head, tail, head_sum, tail_sum, mask = piece
    rows = slice(c * STEP, c * STEP + HALF)
    value = jnp.concatenate([head[rows, :], tail[rows, :]], axis=0)
    mean = (head_sum[c : c + 1, :] + tail_sum[c : c + 1, :]) * (1.0 / SEG)
    shaped = ((value - mean) * window_ref[...]).astype(jnp.bfloat16)
    return (shaped * mask[c : c + 1, :].astype(jnp.bfloat16)).T


def pair_power(lhs, mids, tables, put):
    first_ref, twiddle_ref, second_ref = tables
    for c in range(SUB):
        first = jnp.dot(lhs[c], first_ref[...], preferred_element_type=jnp.float32)
        real, imag = first[:, :RADIX], first[:, RADIX:]
        turn_real, turn_imag = twiddle_ref[0], twiddle_ref[1]
        lanes = slice((c % 2) * RADIX, (c % 2 + 1) * RADIX)
        mids[c // 2, :RADIX, lanes] = (real * turn_real - imag * turn_imag).astype(jnp.bfloat16)
        mids[c // 2, RADIX:, lanes] = (real * turn_imag + imag * turn_real).astype(jnp.bfloat16)
    for i in range(SUB // 2):
        spectrum = jnp.dot(second_ref[...], mids[i], preferred_element_type=jnp.float32)
        real, imag = spectrum[:OUT], spectrum[OUT:]
        power = real * real + imag * imag
        put(2 * i, power[:, :RADIX])
        put(2 * i + 1, power[:, RADIX:])


def own_kernel(where, own, mask, window, out, wide, sums):
    def block(n, _):
        for half in range(2):
            stage(wide.at[half], sums.at[half], own.at[n], half)
        piece = (wide.at[0], wide.at[1], sums.at[0], sums.at[1], mask.at[n, 0])
        for c in range(SUB):
            out[n, c] = shape(c, piece, window)
        return 0

    lax.fori_loop(0, own.shape[0], block, 0)


def local_kernel(
    where, ready, other, mask, first, twiddle, second, window, out, wide, sums, lhs, mids
):
    def block(n, _):
        for half in range(2):
            stage(wide.at[half], sums.at[half], other.at[n], half)
        piece = (wide.at[0], wide.at[1], sums.at[0], sums.at[1], mask.at[n, 0])
        for c in range(SUB):
            lhs[c, :, :RADIX] = ready[n, c]
            lhs[c, :, RADIX:] = shape(c, piece, window)

        def put(c, power):
            out[n, c] = power

        pair_power(lhs, mids, (first, twiddle, second), put)
        return 0

    lax.fori_loop(0, other.shape[0], block, 0)


def cross_kernel(
    groups, where, own, other, lower0, lower1, upper0, upper1, base, weight,
    first, twiddle, second, window, mirror, out,
    load, held, wide, sums, lhs, mids, total, plain, turned, sems, held_sem,
):
    core, chip, group = where[0], where[1], where[2]
    sub = out.shape[0]
    low = group < groups // 2
    high = jnp.logical_not(low)
    rounds = jnp.where(jnp.logical_and(high, chip == groups - 1), 2, 1)
    edge = jnp.where(low, group, group - groups // 2) * sub
    inside = (2 * group + core) * sub

    def copy(source, slot, k):
        return pltpu.make_async_copy(source, load.at[slot, k], sems.at[slot, k])

    def fetch(u):
        slot = u & 1
        n = u // rounds
        again = u - n * rounds == 1
        start = jnp.logical_not(again)
        for index, lo, hi, up, down in (
            (0, own, other, upper0, lower0),
            (1, other, own, upper1, lower1),
        ):
            here = core == index

            @pl.when(jnp.logical_and(here, start))
            def _():
                copy(lo.at[inside + n, pl.ds(HALF, HALF)], slot, 0).start()
                copy(hi.at[inside + n, pl.ds(0, HALF)], slot, 1).start()

            @pl.when(jnp.logical_and(jnp.logical_and(here, start), low))
            def _():
                copy(hi.at[inside + n, pl.ds(HALF, HALF)], slot, 2).start()
                copy(up.at[edge + n], slot, 3).start()

            @pl.when(jnp.logical_and(jnp.logical_and(here, start), high))
            def _():
                copy(down.at[edge + n], slot, 2).start()
                copy(lo.at[inside + n, pl.ds(0, HALF)], slot, 3).start()

            @pl.when(jnp.logical_and(here, again))
            def _():
                copy(hi.at[inside + n, pl.ds(HALF, HALF)], slot, 0).start()
                for k in range(1, 4):
                    copy(up.at[0], slot, k).start()

    held_copy = pltpu.make_async_copy(base.at[pl.ds(group * sub, sub)], held, held_sem)
    fetch(0)
    held_copy.start()
    units = sub * rounds
    lane = lax.broadcasted_iota(jnp.int32, (KBANDS, RADIX), 1)

    def unit(u, _):
        slot = u & 1
        n = u // rounds
        r = u - n * rounds
        again = r == 1

        @pl.when(u + 1 < units)
        def _():
            fetch(u + 1)

        for k in range(4):
            copy(upper0.at[0], slot, k).wait()

        @pl.when(u == 0)
        def _():
            held_copy.wait()

        @pl.when(r == 0)
        def _():
            total[...] = held[n]

        for k in range(4):
            stage(wide.at[k], sums.at[k], load.at[slot, k], 0)
        masks = (jnp.where(again, 3, 1), jnp.where(again, 5, jnp.where(low, 3, 4)))
        for c in range(SUB):
            for s in range(2):
                piece = (
                    wide.at[2 * s], wide.at[2 * s + 1], sums.at[2 * s], sums.at[2 * s + 1],
                    weight.at[n, masks[s]],
                )
                lhs[c, :, s * RADIX : (s + 1) * RADIX] = shape(c, piece, window)

        def put(c, power):
            total[c] = total[c] + power

        pair_power(lhs, mids, (first, twiddle, second), put)

        @pl.when(r == rounds - 1)
        def _():
            for c in range(SUB):
                rows = slice(c * KBANDS, (c + 1) * KBANDS)
                plain[rows, :] = total[c, :KBANDS]
                turned[rows, :] = jnp.where(
                    lane == 0,
                    total[c, KBANDS : 2 * KBANDS],
                    total[c, KBANDS + 1 : 2 * KBANDS + 1],
                )
            plain[SUB * KBANDS :, :] = jnp.sum(weight[n, :4], axis=0)
            turned[SUB * KBANDS :, :] = jnp.zeros((SUB, RADIX), jnp.float32)
            reverse = jnp.dot(
                turned[...].astype(jnp.bfloat16), mirror[...], preferred_element_type=jnp.float32
            )
            out[n] = (plain[...] + reverse).astype(out.dtype)

        return 0

    lax.fori_loop(0, units, unit, 0)


def finish_kernel(keep, *refs):
    *got, scale, out, total = refs
    value = keep[0]
    for piece in got:
        value = value + piece[0].astype(jnp.float32)
    total[...] = value
    inverse = 1.0 / jnp.maximum(total[SUB * KBANDS :, :], 1.0)
    for j in range(KBANDS):
        value = total[pl.ds(j, SUB, stride=KBANDS), :]
        out[:, j * RADIX : (j + 1) * RADIX] = value * scale[j : j + 1, :] * inverse


def whole(array):
    return pl.BlockSpec(array.shape, lambda *_: (0,) * array.ndim)


def per_device(samples, valid):
    first, twiddle, second, window, mirror, scale = make_tables()
    tables = (first, twiddle, second, window)
    channels = samples.shape[0]
    size = lax.axis_size("chan")
    chips = size // 2
    half = chips // 2
    place = lax.axis_index("chan")
    core, chip = place & 1, place >> 1
    sub = channels // (SUB * size)

    def send(value, perm):
        return lax.ppermute(value, "chan", perm)

    def tiled(value):
        return value.reshape(channels // SUB, SUB, RADIX, RADIX).transpose(0, 2, 1, 3)

    swap = [(i, i ^ 1) for i in range(size)]
    links = range(chips - 1)
    tiles = tiled(samples)
    groups = tiles.reshape(chips, 2, sub, RADIX, SUB, RADIX)
    edges = [
        lax.dynamic_slice(
            groups,
            (core * half, c, 0, core * HALF, 0, 0),
            (half, 1, sub, HALF, SUB, RADIX),
        ).reshape(half * sub, HALF, SUB, RADIX)
        for c in range(2)
    ]
    onward = [[(2 * z + 1, 2 * z + 2 + c) for z in links] for c in range(2)]
    back = [[(2 * z + 2, 2 * z + c) for z in links] for c in range(2)]
    lower = [send(edges[c], onward[c]) for c in range(2)]
    upper = [send(edges[c], back[c]) for c in range(2)]
    other = tiled(send(samples, swap))

    theirs = send(valid, swap)
    before = sum(send(valid, onward[c]) for c in range(2))

    def spread(mask):
        count = mask.shape[1]
        mask = mask.astype(jnp.float32).reshape(chips, 2, sub, SUB, count)
        mask = lax.dynamic_index_in_dim(mask, core, 1, False).reshape(chips * sub, SUB, count)
        shape = (chips * sub, count, SUB, RADIX)
        return jnp.broadcast_to(mask.transpose(0, 2, 1)[..., None], shape)

    lo = jnp.where(core == 0, valid, theirs)
    hi = jnp.where(core == 0, theirs, valid)
    last = before[:, 1:]
    weight = spread(jnp.concatenate([lo, hi, last, jnp.zeros_like(last)], axis=1))

    step = 2 if sub % 2 == 0 else 1
    tile = (step, RADIX, SUB, RADIX)
    stripe = STEP * SUB
    half_wide = pltpu.VMEM((2, stripe, RADIX), jnp.float32)
    half_sums = pltpu.VMEM((2, SUB, RADIX), jnp.float32)
    lhs_shape = pltpu.VMEM((SUB, RADIX, 2 * RADIX), jnp.bfloat16)
    mids_shape = pltpu.VMEM((SUB // 2, 2 * RADIX, 2 * RADIX), jnp.bfloat16)
    local_grid = (chips, sub // step)

    def dense(g, i, w):
        return (g * (sub // step) + i, 0, 0, 0)

    def mine(g, i, w):
        return ((2 * g + w[0]) * (sub // step) + i, 0, 0, 0)

    def cost(parts):
        return pl.CostEstimate(
            flops=parts * 50_000 * samples.size // SEG * SEG // RADIX,
            transcendentals=0,
            bytes_accessed=parts * samples.size,
        )

    where = jnp.stack([core, chip]).astype(jnp.int32)
    ready = pl.pallas_call(
        own_kernel,
        grid_spec=pltpu.PrefetchScalarGridSpec(
            num_scalar_prefetch=1,
            grid=local_grid,
            in_specs=[
                pl.BlockSpec(tile, mine),
                pl.BlockSpec((step, 1, SUB, RADIX), dense),
                whole(window),
            ],
            out_specs=pl.BlockSpec((step, SUB, RADIX, RADIX), dense),
            scratch_shapes=[half_wide, half_sums],
        ),
        out_shape=jax.ShapeDtypeStruct((chips * sub, SUB, RADIX, RADIX), jnp.bfloat16),
        cost_estimate=cost(1),
        name="own_segments",
    )(where, tiles, spread(valid[:, :1]), window)
    partial = pl.pallas_call(
        local_kernel,
        grid_spec=pltpu.PrefetchScalarGridSpec(
            num_scalar_prefetch=1,
            grid=local_grid,
            in_specs=[
                pl.BlockSpec((step, SUB, RADIX, RADIX), dense),
                pl.BlockSpec(tile, mine),
                pl.BlockSpec((step, 1, SUB, RADIX), dense),
                *[whole(t) for t in tables],
            ],
            out_specs=pl.BlockSpec((step, SUB, OUT, RADIX), dense),
            scratch_shapes=[half_wide, half_sums, lhs_shape, mids_shape],
        ),
        out_shape=jax.ShapeDtypeStruct((chips * sub, SUB, OUT, RADIX), jnp.float32),
        cost_estimate=cost(3),
        name="local_segments",
    )(where, ready, other, spread(lax.optimization_barrier((theirs, ready))[0][:, :1]), *tables)

    anywhere = pl.BlockSpec(memory_space=pl.ANY)

    def cross(group, dtype):
        return pl.pallas_call(
            functools.partial(cross_kernel, chips),
            grid_spec=pltpu.PrefetchScalarGridSpec(
                num_scalar_prefetch=1,
                grid=(1,),
                in_specs=[
                    *[anywhere] * 7,
                    pl.BlockSpec((sub, SLOTS, SUB, RADIX), lambda i, w: (w[2], 0, 0, 0)),
                    *[whole(t) for t in tables],
                    whole(mirror),
                ],
                out_specs=pl.BlockSpec((sub, ROWS, RADIX), lambda i, w: (0, 0, 0)),
                scratch_shapes=[
                    pltpu.VMEM((2, 4, HALF, SUB, RADIX), jnp.bfloat16),
                    pltpu.VMEM((sub, SUB, OUT, RADIX), jnp.float32),
                    pltpu.VMEM((4, stripe, RADIX), jnp.float32),
                    pltpu.VMEM((4, SUB, RADIX), jnp.float32),
                    lhs_shape,
                    mids_shape,
                    pltpu.VMEM((SUB, OUT, RADIX), jnp.float32),
                    pltpu.VMEM((ROWS, RADIX), jnp.float32),
                    pltpu.VMEM((ROWS, RADIX), jnp.float32),
                    pltpu.SemaphoreType.DMA((2, 4)),
                    pltpu.SemaphoreType.DMA,
                ],
            ),
            out_shape=jax.ShapeDtypeStruct((sub, ROWS, RADIX), dtype),
        )(
            jnp.stack([core, chip, group]).astype(jnp.int32),
            tiles, other, *lower, *upper, partial, weight, *tables, mirror,
        )

    got, after = [], ready
    for shift in sorted(range(1, chips), key=lambda r: -min(r, chips - r)):
        target = (chip + shift) % chips
        target, _ = lax.optimization_barrier((target, after))
        away = cross(target, jnp.bfloat16)
        after = away
        around = [(i, (i + 2 * shift) % size) for i in range(size)]
        got.append(send(away, around))
    chip_last, _ = lax.optimization_barrier((chip, after))
    keep = cross(chip_last, jnp.float32)

    piece = pl.BlockSpec((1, ROWS, RADIX), lambda i: (i, 0, 0))
    return pl.pallas_call(
        finish_kernel,
        grid=(sub,),
        in_specs=[piece] * chips + [whole(scale)],
        out_specs=pl.BlockSpec((SUB, KBANDS * RADIX), lambda i: (i, 0)),
        out_shape=jax.ShapeDtypeStruct((sub * SUB, KBANDS * RADIX), jnp.float32),
        scratch_shapes=[pltpu.VMEM((ROWS, RADIX), jnp.float32)],
        name="finish",
    )(keep, *got, scale)


def solution(mesh):
    return jax.shard_map(
        per_device,
        mesh=mesh,
        in_specs=(P("tm", "chan"), P("tm", "chan")),
        out_specs=P(("tm", "chan"), None),
        check_vma=False,
    )
```

```python
import functools

import jax
import jax.numpy as jnp
import numpy as np
from jax import lax
from jax.experimental import pallas as pl
from jax.experimental.pallas import tpu as pltpu
from jax.sharding import PartitionSpec as P


RADIX = 128
KBANDS = 33
SUB = 8
HALF = RADIX // 2
STEP = HALF + 4
OUT = 72
ROWS = SUB * KBANDS + SUB
SEG = RADIX * RADIX


def make_tables():
    counter = np.arange(RADIX)
    angle = 2 * np.pi * ((counter[:, None] * counter[None, :]) % RADIX) / RADIX
    cos, sin = np.cos(angle), np.sin(angle)
    first = np.block([[cos, -sin], [sin, cos]])
    mid = 2 * np.pi * (counter[:, None] * counter[None, :]) / SEG
    twiddle = np.stack([np.cos(mid), -np.sin(mid)])
    bands = np.concatenate([np.arange(KBANDS), RADIX - np.arange(KBANDS + 1)]) % RADIX
    second = np.zeros((2 * OUT, 2 * RADIX))
    size = len(bands)
    second[:size, :RADIX], second[:size, RADIX:] = cos[bands], sin[bands]
    second[OUT : OUT + size, :RADIX], second[OUT : OUT + size, RADIX:] = -sin[bands], cos[bands]
    window = (0.5 - 0.5 * np.cos(2 * np.pi * np.arange(SEG) / SEG)).astype(np.float32)
    mirror = np.zeros((RADIX, RADIX))
    mirror[(RADIX - counter) % RADIX, counter] = 1.0
    scale = np.full((KBANDS, RADIX), 2.0)
    scale[0, 0] = 1.0
    scale = 0.5 * scale / np.sum(window.astype(np.float64) ** 2)
    return (
        jnp.asarray(first, jnp.bfloat16),
        jnp.asarray(twiddle, jnp.float32),
        jnp.asarray(second, jnp.bfloat16),
        jnp.asarray(window.reshape(RADIX, RADIX)),
        jnp.asarray(mirror, jnp.bfloat16),
        jnp.asarray(scale, jnp.float32),
    )


def stage(dst, sums, source, half):
    total = [None] * 4
    for a in range(HALF):
        value = source[half * HALF + a].astype(jnp.float32)
        dst[pl.ds(a, SUB, stride=STEP), :] = value
        total[a % 4] = value if total[a % 4] is None else total[a % 4] + value
    total = (total[0] + total[1]) + (total[2] + total[3])
    sums[...] = jnp.broadcast_to(jnp.sum(total, axis=1, keepdims=True), (SUB, RADIX))


def shape(c, piece, window_ref):
    head, tail, head_sum, tail_sum, mask = piece
    rows = slice(c * STEP, c * STEP + HALF)
    value = jnp.concatenate([head[rows, :], tail[rows, :]], axis=0)
    mean = (head_sum[c : c + 1, :] + tail_sum[c : c + 1, :]) * (1.0 / SEG)
    shaped = ((value - mean) * window_ref[...]).astype(jnp.bfloat16)
    return (shaped * mask[c : c + 1, :].astype(jnp.bfloat16)).T


def pair_power(lhs, mids, tables, put):
    first_ref, twiddle_ref, second_ref = tables
    for c in range(SUB):
        first = jnp.dot(lhs[c], first_ref[...], preferred_element_type=jnp.float32)
        real, imag = first[:, :RADIX], first[:, RADIX:]
        turn_real, turn_imag = twiddle_ref[0], twiddle_ref[1]
        lanes = slice((c % 2) * RADIX, (c % 2 + 1) * RADIX)
        mids[c // 2, :RADIX, lanes] = (real * turn_real - imag * turn_imag).astype(jnp.bfloat16)
        mids[c // 2, RADIX:, lanes] = (real * turn_imag + imag * turn_real).astype(jnp.bfloat16)
    for i in range(SUB // 2):
        spectrum = jnp.dot(second_ref[...], mids[i], preferred_element_type=jnp.float32)
        real, imag = spectrum[:OUT], spectrum[OUT:]
        power = real * real + imag * imag
        put(2 * i, power[:, :RADIX])
        put(2 * i + 1, power[:, RADIX:])


def local_kernel(
    where, own, other, mask, first, twiddle, second, window, out, wide, sums, lhs, mids
):
    def block(n, _):
        for half in range(2):
            stage(wide.at[half], sums.at[half], own.at[n], half)
            stage(wide.at[2 + half], sums.at[2 + half], other.at[n], half)
        for c in range(SUB):
            for s in range(2):
                piece = (
                    wide.at[2 * s], wide.at[2 * s + 1], sums.at[2 * s], sums.at[2 * s + 1],
                    mask.at[n, s],
                )
                lhs[c, :, s * RADIX : (s + 1) * RADIX] = shape(c, piece, window)

        def put(c, power):
            out[n, c] = power

        pair_power(lhs, mids, (first, twiddle, second), put)
        return 0

    lax.fori_loop(0, own.shape[0], block, 0)


def cross_kernel(
    groups, sub, count, where, own, other, lower0, lower1, upper0, upper1, base, weight,
    first, twiddle, second, window, mirror, *rest,
):
    outs = rest[:count]
    load, held, wide, sums, lhs, mids, total, plain, turned, sems, held_sems = rest[count:]
    core, chip = where[0], where[1]

    def facts(i):
        group = where[2 + i]
        low = group < groups // 2
        last = jnp.logical_and(jnp.logical_not(low), chip == groups - 1)
        return group, low, jnp.where(last, 2, 1)

    starts = [jnp.int32(0)]
    for i in range(count):
        starts.append(starts[-1] + sub * facts(i)[2])
    units = starts[-1]

    def find(u):
        index = jnp.int32(0)
        start = jnp.int32(0)
        for i in range(1, count):
            index = jnp.where(u >= starts[i], i, index)
            start = jnp.where(u >= starts[i], starts[i], start)
        group, low, rounds = facts(index)
        n = (u - start) >> (rounds - 1)
        again = jnp.logical_and(rounds == 2, ((u - start) & 1) == 1)
        final = jnp.logical_or(rounds == 1, again)
        return index, group, low, n, again, final

    def copy(source, slot, k):
        return pltpu.make_async_copy(source, load.at[slot, k], sems.at[slot, k])

    def fetch(u):
        slot = u & 1
        _, group, low, n, again, _ = find(u)
        start = jnp.logical_not(again)
        high = jnp.logical_not(low)
        edge = jnp.where(low, group, group - groups // 2) * sub
        inside = (2 * group + core) * sub
        for index, lo, hi, up, down in (
            (0, own, other, upper0, lower0),
            (1, other, own, upper1, lower1),
        ):
            here = core == index

            @pl.when(jnp.logical_and(here, start))
            def _():
                copy(lo.at[inside + n, pl.ds(HALF, HALF)], slot, 0).start()
                copy(hi.at[inside + n, pl.ds(0, HALF)], slot, 1).start()

            @pl.when(jnp.logical_and(jnp.logical_and(here, start), low))
            def _():
                copy(hi.at[inside + n, pl.ds(HALF, HALF)], slot, 2).start()
                copy(up.at[edge + n], slot, 3).start()

            @pl.when(jnp.logical_and(jnp.logical_and(here, start), high))
            def _():
                copy(down.at[edge + n], slot, 2).start()
                copy(lo.at[inside + n, pl.ds(0, HALF)], slot, 3).start()

            @pl.when(jnp.logical_and(here, again))
            def _():
                copy(hi.at[inside + n, pl.ds(HALF, HALF)], slot, 0).start()
                for k in range(1, 4):
                    copy(up.at[0], slot, k).start()

    held_copies = [
        pltpu.make_async_copy(base.at[pl.ds(where[2 + i] * sub, sub)], held.at[i], held_sems.at[i])
        for i in range(count)
    ]
    fetch(0)
    for held_copy in held_copies:
        held_copy.start()
    lane = lax.broadcasted_iota(jnp.int32, (KBANDS, RADIX), 1)

    def unit(u, _):
        slot = u & 1
        index, group, low, n, again, final = find(u)

        @pl.when(u + 1 < units)
        def _():
            fetch(u + 1)

        for k in range(4):
            copy(upper0.at[0], slot, k).wait()

        @pl.when(u == 0)
        def _():
            for held_copy in held_copies:
                held_copy.wait()

        @pl.when(jnp.logical_not(again))
        def _():
            total[...] = held[index, n]

        row = group * sub + n
        for k in range(4):
            stage(wide.at[k], sums.at[k], load.at[slot, k], 0)
        masks = (jnp.where(again, 3, 1), jnp.where(again, 5, jnp.where(low, 3, 4)))
        for c in range(SUB):
            for s in range(2):
                piece = (
                    wide.at[2 * s], wide.at[2 * s + 1], sums.at[2 * s], sums.at[2 * s + 1],
                    weight.at[row, masks[s]],
                )
                lhs[c, :, s * RADIX : (s + 1) * RADIX] = shape(c, piece, window)

        def put(c, power):
            total[c] = total[c] + power

        pair_power(lhs, mids, (first, twiddle, second), put)

        @pl.when(final)
        def _():
            for c in range(SUB):
                rows = slice(c * KBANDS, (c + 1) * KBANDS)
                plain[rows, :] = total[c, :KBANDS]
                turned[rows, :] = jnp.where(
                    lane == 0,
                    total[c, KBANDS : 2 * KBANDS],
                    total[c, KBANDS + 1 : 2 * KBANDS + 1],
                )
            plain[SUB * KBANDS :, :] = jnp.sum(weight[row, :4], axis=0)
            turned[SUB * KBANDS :, :] = jnp.zeros((SUB, RADIX), jnp.float32)
            reverse = jnp.dot(
                turned[...].astype(jnp.bfloat16), mirror[...], preferred_element_type=jnp.float32
            )
            packed = (plain[...] + reverse).astype(jnp.bfloat16)
            for i, out in enumerate(outs):

                @pl.when(index == i)
                def _():
                    out[n] = packed

        return 0

    lax.fori_loop(0, units, unit, 0)


def finish_kernel(*refs):
    *pieces, scale, out, total = refs
    for n in range(out.shape[0] // SUB):
        value = pieces[0][n].astype(jnp.float32)
        for piece in pieces[1:]:
            value = value + piece[n].astype(jnp.float32)
        total[...] = value
        inverse = 1.0 / jnp.maximum(total[SUB * KBANDS :, :], 1.0)
        for j in range(KBANDS):
            value = total[pl.ds(j, SUB, stride=KBANDS), :]
            out[n * SUB : (n + 1) * SUB, j * RADIX : (j + 1) * RADIX] = (
                value * scale[j : j + 1, :] * inverse
            )


def whole(array):
    return pl.BlockSpec(array.shape, lambda *_: (0,) * array.ndim)


def per_device(samples, valid):
    first, twiddle, second, window, mirror, scale = make_tables()
    tables = (first, twiddle, second, window)
    channels = samples.shape[0]
    size = lax.axis_size("chan")
    chips = size // 2
    half = chips // 2
    place = lax.axis_index("chan")
    core, chip = place & 1, place >> 1
    sub = channels // (SUB * size)

    def send(value, perm):
        return lax.ppermute(value, "chan", perm)

    def tiled(value):
        return value.reshape(channels // SUB, SUB, RADIX, RADIX).transpose(0, 2, 1, 3)

    swap = [(i, i ^ 1) for i in range(size)]
    links = range(chips - 1)
    tiles = tiled(samples)
    groups = tiles.reshape(chips, 2, sub, RADIX, SUB, RADIX)
    edges = [
        lax.dynamic_slice(
            groups,
            (core * half, c, 0, core * HALF, 0, 0),
            (half, 1, sub, HALF, SUB, RADIX),
        ).reshape(half * sub, HALF, SUB, RADIX)
        for c in range(2)
    ]
    onward = [[(2 * z + 1, 2 * z + 2 + c) for z in links] for c in range(2)]
    back = [[(2 * z + 2, 2 * z + c) for z in links] for c in range(2)]
    lower = [send(edges[c], onward[c]) for c in range(2)]
    upper = [send(edges[c], back[c]) for c in range(2)]
    other = tiled(send(samples, swap))

    theirs = send(valid, swap)
    before = sum(send(valid, onward[c]) for c in range(2))

    def spread(mask):
        count = mask.shape[1]
        mask = mask.astype(jnp.float32).reshape(chips, 2, sub, SUB, count)
        mask = lax.dynamic_index_in_dim(mask, core, 1, False).reshape(chips * sub, SUB, count)
        shape = (chips * sub, count, SUB, RADIX)
        return jnp.broadcast_to(mask.transpose(0, 2, 1)[..., None], shape)

    lo = jnp.where(core == 0, valid, theirs)
    hi = jnp.where(core == 0, theirs, valid)
    last = before[:, 1:]
    weight = spread(jnp.concatenate([lo, hi, last, jnp.zeros_like(last)], axis=1))

    step = 2 if sub % 2 == 0 else 1
    tile = (step, RADIX, SUB, RADIX)
    stripe = STEP * SUB
    wide_shape = pltpu.VMEM((4, stripe, RADIX), jnp.float32)
    sums_shape = pltpu.VMEM((4, SUB, RADIX), jnp.float32)
    lhs_shape = pltpu.VMEM((SUB, RADIX, 2 * RADIX), jnp.bfloat16)
    mids_shape = pltpu.VMEM((SUB // 2, 2 * RADIX, 2 * RADIX), jnp.bfloat16)
    local_grid = (chips, sub // step)

    def dense(g, i, w):
        return (g * (sub // step) + i, 0, 0, 0)

    def mine(g, i, w):
        return ((2 * g + w[0]) * (sub // step) + i, 0, 0, 0)

    where = jnp.stack([core, chip]).astype(jnp.int32)
    partial = pl.pallas_call(
        local_kernel,
        grid_spec=pltpu.PrefetchScalarGridSpec(
            num_scalar_prefetch=1,
            grid=local_grid,
            in_specs=[
                pl.BlockSpec(tile, mine),
                pl.BlockSpec(tile, mine),
                pl.BlockSpec((step, 2, SUB, RADIX), dense),
                *[whole(t) for t in tables],
            ],
            out_specs=pl.BlockSpec((step, SUB, OUT, RADIX), dense),
            scratch_shapes=[wide_shape, sums_shape, lhs_shape, mids_shape],
        ),
        out_shape=jax.ShapeDtypeStruct((chips * sub, SUB, OUT, RADIX), jnp.float32),
        name="local_segments",
    )(where, tiles, other, spread(jnp.concatenate([valid[:, :1], theirs[:, :1]], axis=1)), *tables)

    anywhere = pl.BlockSpec(memory_space=pl.ANY)

    def cross(targets):
        count = len(targets)
        return pl.pallas_call(
            functools.partial(cross_kernel, chips, sub, count),
            grid_spec=pltpu.PrefetchScalarGridSpec(
                num_scalar_prefetch=1,
                grid=(1,),
                in_specs=[
                    *[anywhere] * 7,
                    whole(weight),
                    *[whole(t) for t in tables],
                    whole(mirror),
                ],
                out_specs=[pl.BlockSpec((sub, ROWS, RADIX), lambda i, w: (0, 0, 0))] * count,
                scratch_shapes=[
                    pltpu.VMEM((2, 4, HALF, SUB, RADIX), jnp.bfloat16),
                    pltpu.VMEM((count, sub, SUB, OUT, RADIX), jnp.float32),
                    wide_shape,
                    sums_shape,
                    lhs_shape,
                    mids_shape,
                    pltpu.VMEM((SUB, OUT, RADIX), jnp.float32),
                    pltpu.VMEM((ROWS, RADIX), jnp.float32),
                    pltpu.VMEM((ROWS, RADIX), jnp.float32),
                    pltpu.SemaphoreType.DMA((2, 4)),
                    pltpu.SemaphoreType.DMA((count,)),
                ],
            ),
            out_shape=[jax.ShapeDtypeStruct((sub, ROWS, RADIX), jnp.bfloat16)] * count,
        )(
            jnp.stack([core, chip, *targets]).astype(jnp.int32),
            tiles, other, *lower, *upper, partial, weight, *tables, mirror,
        )

    shifts = sorted(range(1, chips), key=lambda r: (-min(r, chips - r), r)) + [0]
    targets = [jnp.where(chip + r >= chips, chip + r - chips, chip + r) for r in shifts]
    early = cross(targets[:half])
    rest, _ = lax.optimization_barrier((jnp.stack(targets[half:]), early[-1]))
    late = cross([rest[i] for i in range(chips - half)])
    pieces = [*early, *late]
    for k, shift in enumerate(shifts[:-1]):
        around = [(i, (i + 2 * shift) % size) for i in range(size)]
        pieces[k] = send(pieces[k], around)

    return pl.pallas_call(
        finish_kernel,
        out_shape=jax.ShapeDtypeStruct((sub * SUB, KBANDS * RADIX), jnp.float32),
        scratch_shapes=[pltpu.VMEM((ROWS, RADIX), jnp.float32)],
        name="finish",
    )(*pieces, scale)


def solution(mesh):
    return jax.shard_map(
        per_device,
        mesh=mesh,
        in_specs=(P("tm", "chan"), P("tm", "chan")),
        out_specs=P(("tm", "chan"), None),
        check_vma=False,
    )
```

```python
import functools

import jax
import jax.numpy as jnp
import numpy as np
from jax import lax
from jax.experimental import pallas as pl
from jax.experimental.pallas import tpu as pltpu
from jax.sharding import PartitionSpec as P


RADIX = 128
KBANDS = 33
SUB = 8
HALF = RADIX // 2
STEP = HALF + 4
OUT = 72
ROWS = SUB * KBANDS + SUB
SEG = RADIX * RADIX


def make_tables():
    counter = np.arange(RADIX)
    angle = 2 * np.pi * ((counter[:, None] * counter[None, :]) % RADIX) / RADIX
    cos, sin = np.cos(angle), np.sin(angle)
    first = np.block([[cos, -sin], [sin, cos]])
    mid = 2 * np.pi * (counter[:, None] * counter[None, :]) / SEG
    twiddle = np.stack([np.cos(mid), -np.sin(mid)])
    bands = np.concatenate([np.arange(KBANDS), RADIX - np.arange(KBANDS + 1)]) % RADIX
    second = np.zeros((2 * OUT, 2 * RADIX))
    size = len(bands)
    second[:size, :RADIX], second[:size, RADIX:] = cos[bands], sin[bands]
    second[OUT : OUT + size, :RADIX], second[OUT : OUT + size, RADIX:] = -sin[bands], cos[bands]
    window = (0.5 - 0.5 * np.cos(2 * np.pi * np.arange(SEG) / SEG)).astype(np.float32)
    mirror = np.zeros((RADIX, RADIX))
    mirror[(RADIX - counter) % RADIX, counter] = 1.0
    scale = np.full((KBANDS, RADIX), 2.0)
    scale[0, 0] = 1.0
    scale = 0.5 * scale / np.sum(window.astype(np.float64) ** 2)
    return (
        jnp.asarray(first, jnp.bfloat16),
        jnp.asarray(twiddle, jnp.float32),
        jnp.asarray(second, jnp.bfloat16),
        jnp.asarray(window.reshape(RADIX, RADIX)),
        jnp.asarray(mirror, jnp.bfloat16),
        jnp.asarray(scale, jnp.float32),
    )


def stage(dst, sums, source, half):
    total = [None] * 4
    for a in range(HALF):
        value = source[half * HALF + a].astype(jnp.float32)
        dst[pl.ds(a, SUB, stride=STEP), :] = value
        total[a % 4] = value if total[a % 4] is None else total[a % 4] + value
    total = (total[0] + total[1]) + (total[2] + total[3])
    sums[...] = jnp.broadcast_to(jnp.sum(total, axis=1, keepdims=True), (SUB, RADIX))


def shape(c, piece, window_ref):
    head, tail, head_sum, tail_sum, mask = piece
    rows = slice(c * STEP, c * STEP + HALF)
    value = jnp.concatenate([head[rows, :], tail[rows, :]], axis=0)
    mean = (head_sum[c : c + 1, :] + tail_sum[c : c + 1, :]) * (1.0 / SEG)
    shaped = ((value - mean) * window_ref[...]).astype(jnp.bfloat16)
    return (shaped * mask[c : c + 1, :].astype(jnp.bfloat16)).T


def pair_power(lhs, mids, tables, put):
    first_ref, twiddle_ref, second_ref = tables
    for c in range(SUB):
        first = jnp.dot(lhs[c], first_ref[...], preferred_element_type=jnp.float32)
        real, imag = first[:, :RADIX], first[:, RADIX:]
        turn_real, turn_imag = twiddle_ref[0], twiddle_ref[1]
        lanes = slice((c % 2) * RADIX, (c % 2 + 1) * RADIX)
        mids[c // 2, :RADIX, lanes] = (real * turn_real - imag * turn_imag).astype(jnp.bfloat16)
        mids[c // 2, RADIX:, lanes] = (real * turn_imag + imag * turn_real).astype(jnp.bfloat16)
    for i in range(SUB // 2):
        spectrum = jnp.dot(second_ref[...], mids[i], preferred_element_type=jnp.float32)
        real, imag = spectrum[:OUT], spectrum[OUT:]
        power = real * real + imag * imag
        put(2 * i, power[:, :RADIX])
        put(2 * i + 1, power[:, RADIX:])


def local_kernel(
    groups, where, own, other, mask, first, twiddle, second, window, out, wide, sums, lhs, mids
):
    core, chip = where[0], where[1]
    ending = jnp.logical_and(chip == groups - 1, pl.program_id(0) >= groups // 2)
    tables = (first, twiddle, second)

    def block(n, _):
        for half in range(2):
            stage(wide.at[half], sums.at[half], own.at[n], half)
            stage(wide.at[2 + half], sums.at[2 + half], other.at[n], half)
        for c in range(SUB):
            for s in range(2):
                piece = (
                    wide.at[2 * s], wide.at[2 * s + 1], sums.at[2 * s], sums.at[2 * s + 1],
                    mask.at[n, s],
                )
                lhs[c, :, s * RADIX : (s + 1) * RADIX] = shape(c, piece, window)

        def put(c, power):
            out[n, c] = power

        pair_power(lhs, mids, tables, put)

        @pl.when(ending)
        def _():
            head = jnp.where(core == 1, 1, 3)
            tail = 4 - head
            wide[tail] = jnp.zeros_like(wide[tail])
            sums[tail] = jnp.zeros_like(sums[tail])
            piece = (wide.at[head], wide.at[tail], sums.at[head], sums.at[tail], mask.at[n, 2])
            for c in range(SUB):
                lhs[c, :, :RADIX] = shape(c, piece, window)
                lhs[c, :, RADIX:] = jnp.zeros((RADIX, RADIX), jnp.bfloat16)

            def add(c, power):
                out[n, c] = out[n, c] + power

            pair_power(lhs, mids, tables, add)

        return 0

    lax.fori_loop(0, own.shape[0], block, 0)


def cross_kernel(
    groups, sub, count, where, own, other, lower0, lower1, upper0, upper1, base, weight,
    first, twiddle, second, window, mirror, *rest,
):
    outs = rest[:count]
    load, held, wide, sums, lhs, mids, total, plain, turned, sems, held_sems = rest[count:]
    core = where[0]

    units = count * sub

    def find(u):
        index = u // sub
        group = where[2 + index]
        return index, group, group < groups // 2, u - index * sub

    def copy(source, slot, k):
        return pltpu.make_async_copy(source, load.at[slot, k], sems.at[slot, k])

    def fetch(u):
        slot = u & 1
        _, group, low, n = find(u)
        high = jnp.logical_not(low)
        edge = jnp.where(low, group, group - groups // 2) * sub
        inside = (2 * group + core) * sub
        for index, lo, hi, up, down in (
            (0, own, other, upper0, lower0),
            (1, other, own, upper1, lower1),
        ):
            here = core == index

            @pl.when(here)
            def _():
                copy(lo.at[inside + n, pl.ds(HALF, HALF)], slot, 0).start()
                copy(hi.at[inside + n, pl.ds(0, HALF)], slot, 1).start()

            @pl.when(jnp.logical_and(here, low))
            def _():
                copy(hi.at[inside + n, pl.ds(HALF, HALF)], slot, 2).start()
                copy(up.at[edge + n], slot, 3).start()

            @pl.when(jnp.logical_and(here, high))
            def _():
                copy(down.at[edge + n], slot, 2).start()
                copy(lo.at[inside + n, pl.ds(0, HALF)], slot, 3).start()

    held_copies = [
        pltpu.make_async_copy(base.at[pl.ds(where[2 + i] * sub, sub)], held.at[i], held_sems.at[i])
        for i in range(count)
    ]
    fetch(0)
    for held_copy in held_copies:
        held_copy.start()
    lane = lax.broadcasted_iota(jnp.int32, (KBANDS, RADIX), 1)

    def unit(u, _):
        slot = u & 1
        index, group, low, n = find(u)

        @pl.when(u + 1 < units)
        def _():
            fetch(u + 1)

        for k in range(4):
            copy(upper0.at[0], slot, k).wait()

        @pl.when(u == 0)
        def _():
            for held_copy in held_copies:
                held_copy.wait()

        total[...] = held[index, n]
        row = group * sub + n
        for k in range(4):
            stage(wide.at[k], sums.at[k], load.at[slot, k], 0)
        masks = (1, jnp.where(low, 3, 4))
        for c in range(SUB):
            for s in range(2):
                piece = (
                    wide.at[2 * s], wide.at[2 * s + 1], sums.at[2 * s], sums.at[2 * s + 1],
                    weight.at[row, masks[s]],
                )
                lhs[c, :, s * RADIX : (s + 1) * RADIX] = shape(c, piece, window)

        def put(c, power):
            total[c] = total[c] + power

        pair_power(lhs, mids, (first, twiddle, second), put)

        for c in range(SUB):
            rows = slice(c * KBANDS, (c + 1) * KBANDS)
            plain[rows, :] = total[c, :KBANDS]
            turned[rows, :] = jnp.where(
                lane == 0,
                total[c, KBANDS : 2 * KBANDS],
                total[c, KBANDS + 1 : 2 * KBANDS + 1],
            )
        plain[SUB * KBANDS :, :] = jnp.sum(weight[row, :4], axis=0)
        turned[SUB * KBANDS :, :] = jnp.zeros((SUB, RADIX), jnp.float32)
        reverse = jnp.dot(
            turned[...].astype(jnp.bfloat16), mirror[...], preferred_element_type=jnp.float32
        )
        packed = (plain[...] + reverse).astype(jnp.bfloat16)
        for i, out in enumerate(outs):

            @pl.when(index == i)
            def _():
                out[n] = packed

        return 0

    lax.fori_loop(0, units, unit, 0)


def finish_kernel(*refs):
    *pieces, scale, out, total = refs
    for n in range(out.shape[0] // SUB):
        value = pieces[0][n].astype(jnp.float32)
        for piece in pieces[1:]:
            value = value + piece[n].astype(jnp.float32)
        total[...] = value
        inverse = 1.0 / jnp.maximum(total[SUB * KBANDS :, :], 1.0)
        for j in range(KBANDS):
            value = total[pl.ds(j, SUB, stride=KBANDS), :]
            out[n * SUB : (n + 1) * SUB, j * RADIX : (j + 1) * RADIX] = (
                value * scale[j : j + 1, :] * inverse
            )


def whole(array):
    return pl.BlockSpec(array.shape, lambda *_: (0,) * array.ndim)


def per_device(samples, valid):
    first, twiddle, second, window, mirror, scale = make_tables()
    tables = (first, twiddle, second, window)
    channels = samples.shape[0]
    size = lax.axis_size("chan")
    chips = size // 2
    half = chips // 2
    place = lax.axis_index("chan")
    core, chip = place & 1, place >> 1
    sub = channels // (SUB * size)

    def send(value, perm):
        return lax.ppermute(value, "chan", perm)

    def tiled(value):
        return value.reshape(channels // SUB, SUB, RADIX, RADIX).transpose(0, 2, 1, 3)

    swap = [(i, i ^ 1) for i in range(size)]
    links = range(chips - 1)
    tiles = tiled(samples)
    groups = tiles.reshape(chips, 2, sub, RADIX, SUB, RADIX)
    edges = [
        lax.dynamic_slice(
            groups,
            (core * half, c, 0, core * HALF, 0, 0),
            (half, 1, sub, HALF, SUB, RADIX),
        ).reshape(half * sub, HALF, SUB, RADIX)
        for c in range(2)
    ]
    onward = [[(2 * z + 1, 2 * z + 2 + c) for z in links] for c in range(2)]
    back = [[(2 * z + 2, 2 * z + c) for z in links] for c in range(2)]
    lower = [send(edges[c], onward[c]) for c in range(2)]
    upper = [send(edges[c], back[c]) for c in range(2)]
    other = tiled(send(samples, swap))

    theirs = send(valid, swap)
    before = sum(send(valid, onward[c]) for c in range(2))

    def spread(mask):
        count = mask.shape[1]
        mask = mask.astype(jnp.float32).reshape(chips, 2, sub, SUB, count)
        mask = lax.dynamic_index_in_dim(mask, core, 1, False).reshape(chips * sub, SUB, count)
        shape = (chips * sub, count, SUB, RADIX)
        return jnp.broadcast_to(mask.transpose(0, 2, 1)[..., None], shape)

    lo = jnp.where(core == 0, valid, theirs)
    hi = jnp.where(core == 0, theirs, valid)
    step = 2 if sub % 2 == 0 else 1
    tile = (step, RADIX, SUB, RADIX)
    stripe = STEP * SUB
    wide_shape = pltpu.VMEM((4, stripe, RADIX), jnp.float32)
    sums_shape = pltpu.VMEM((4, SUB, RADIX), jnp.float32)
    lhs_shape = pltpu.VMEM((SUB, RADIX, 2 * RADIX), jnp.bfloat16)
    mids_shape = pltpu.VMEM((SUB // 2, 2 * RADIX, 2 * RADIX), jnp.bfloat16)
    local_grid = (chips, sub // step)

    def dense(g, i, w):
        return (g * (sub // step) + i, 0, 0, 0)

    def mine(g, i, w):
        return ((2 * g + w[0]) * (sub // step) + i, 0, 0, 0)

    local_mask = spread(jnp.concatenate([valid[:, :1], theirs[:, :1], hi[:, 1:]], axis=1))
    where = jnp.stack([core, chip]).astype(jnp.int32)
    partial = pl.pallas_call(
        functools.partial(local_kernel, chips),
        grid_spec=pltpu.PrefetchScalarGridSpec(
            num_scalar_prefetch=1,
            grid=local_grid,
            in_specs=[
                pl.BlockSpec(tile, mine),
                pl.BlockSpec(tile, mine),
                pl.BlockSpec((step, 3, SUB, RADIX), dense),
                *[whole(t) for t in tables],
            ],
            out_specs=pl.BlockSpec((step, SUB, OUT, RADIX), dense),
            scratch_shapes=[wide_shape, sums_shape, lhs_shape, mids_shape],
        ),
        out_shape=jax.ShapeDtypeStruct((chips * sub, SUB, OUT, RADIX), jnp.float32),
        name="local_segments",
    )(where, tiles, other, local_mask, *tables)

    before, _ = lax.optimization_barrier((before, partial))
    weight = spread(jnp.concatenate([lo, hi, before[:, 1:]], axis=1))

    anywhere = pl.BlockSpec(memory_space=pl.ANY)

    def cross(targets):
        count = len(targets)
        return pl.pallas_call(
            functools.partial(cross_kernel, chips, sub, count),
            grid_spec=pltpu.PrefetchScalarGridSpec(
                num_scalar_prefetch=1,
                grid=(1,),
                in_specs=[
                    *[anywhere] * 7,
                    whole(weight),
                    *[whole(t) for t in tables],
                    whole(mirror),
                ],
                out_specs=[pl.BlockSpec((sub, ROWS, RADIX), lambda i, w: (0, 0, 0))] * count,
                scratch_shapes=[
                    pltpu.VMEM((2, 4, HALF, SUB, RADIX), jnp.bfloat16),
                    pltpu.VMEM((count, sub, SUB, OUT, RADIX), jnp.float32),
                    wide_shape,
                    sums_shape,
                    lhs_shape,
                    mids_shape,
                    pltpu.VMEM((SUB, OUT, RADIX), jnp.float32),
                    pltpu.VMEM((ROWS, RADIX), jnp.float32),
                    pltpu.VMEM((ROWS, RADIX), jnp.float32),
                    pltpu.SemaphoreType.DMA((2, 4)),
                    pltpu.SemaphoreType.DMA((count,)),
                ],
            ),
            out_shape=[jax.ShapeDtypeStruct((sub, ROWS, RADIX), jnp.bfloat16)] * count,
        )(
            jnp.stack([core, chip, *targets]).astype(jnp.int32),
            tiles, other, *lower, *upper, partial, weight, *tables, mirror,
        )

    shifts = sorted(range(1, chips), key=lambda r: (-min(r, chips - r), r)) + [0]
    targets = [jnp.where(chip + r >= chips, chip + r - chips, chip + r) for r in shifts]
    early = cross(targets[:half])
    rest, _ = lax.optimization_barrier((jnp.stack(targets[half:]), early[-1]))
    late = cross([rest[i] for i in range(chips - half)])
    pieces = [*early, *late]
    for k, shift in enumerate(shifts[:-1]):
        around = [(i, (i + 2 * shift) % size) for i in range(size)]
        pieces[k] = send(pieces[k], around)

    return pl.pallas_call(
        finish_kernel,
        out_shape=jax.ShapeDtypeStruct((sub * SUB, KBANDS * RADIX), jnp.float32),
        scratch_shapes=[pltpu.VMEM((ROWS, RADIX), jnp.float32)],
        name="finish",
    )(*pieces, scale)


def solution(mesh):
    return jax.shard_map(
        per_device,
        mesh=mesh,
        in_specs=(P("tm", "chan"), P("tm", "chan")),
        out_specs=P(("tm", "chan"), None),
        check_vma=False,
    )
```

```python
import functools

import jax
import jax.numpy as jnp
import numpy as np
from jax import lax
from jax.experimental import pallas as pl
from jax.experimental.pallas import tpu as pltpu
from jax.sharding import PartitionSpec as P


RADIX = 128
KBANDS = 33
SUB = 8
HALF = RADIX // 2
STEP = HALF + 4
OUT = 72
ROWS = SUB * KBANDS + SUB
SEG = RADIX * RADIX
DEPTH = 4


def make_tables():
    counter = np.arange(RADIX)
    angle = 2 * np.pi * ((counter[:, None] * counter[None, :]) % RADIX) / RADIX
    cos, sin = np.cos(angle), np.sin(angle)
    first = np.block([[cos, -sin], [sin, cos]])
    mid = 2 * np.pi * (counter[:, None] * counter[None, :]) / SEG
    twiddle = np.stack([np.cos(mid), -np.sin(mid)])
    bands = np.concatenate([np.arange(KBANDS), RADIX - np.arange(KBANDS + 1)]) % RADIX
    second = np.zeros((2 * OUT, 2 * RADIX))
    size = len(bands)
    second[:size, :RADIX], second[:size, RADIX:] = cos[bands], sin[bands]
    second[OUT : OUT + size, :RADIX], second[OUT : OUT + size, RADIX:] = -sin[bands], cos[bands]
    window = (0.5 - 0.5 * np.cos(2 * np.pi * np.arange(SEG) / SEG)).astype(np.float32)
    mirror = np.zeros((RADIX, RADIX))
    mirror[(RADIX - counter) % RADIX, counter] = 1.0
    scale = np.full((KBANDS, RADIX), 2.0)
    scale[0, 0] = 1.0
    scale = 0.5 * scale / np.sum(window.astype(np.float64) ** 2)
    return (
        jnp.asarray(first, jnp.bfloat16),
        jnp.asarray(twiddle, jnp.float32),
        jnp.asarray(second, jnp.bfloat16),
        jnp.asarray(window.reshape(RADIX, RADIX)),
        jnp.asarray(mirror, jnp.bfloat16),
        jnp.asarray(scale, jnp.float32),
    )


def stage(dst, sums, source, half):
    total = [None] * 4
    for a in range(HALF):
        value = source[half * HALF + a].astype(jnp.float32)
        dst[pl.ds(a, SUB, stride=STEP), :] = value
        total[a % 4] = value if total[a % 4] is None else total[a % 4] + value
    total = (total[0] + total[1]) + (total[2] + total[3])
    sums[...] = jnp.broadcast_to(jnp.sum(total, axis=1, keepdims=True), (SUB, RADIX))


def shape(c, piece, window_ref):
    head, tail, head_sum, tail_sum, mask = piece
    rows = slice(c * STEP, c * STEP + HALF)
    value = jnp.concatenate([head[rows, :], tail[rows, :]], axis=0)
    mean = (head_sum[c : c + 1, :] + tail_sum[c : c + 1, :]) * (1.0 / SEG)
    shaped = ((value - mean) * window_ref[...]).astype(jnp.bfloat16)
    return (shaped * mask[c : c + 1, :].astype(jnp.bfloat16)).T


def pair_power(lhs, mids, tables, put):
    first_ref, twiddle_ref, second_ref = tables
    for c in range(SUB):
        first = jnp.dot(lhs[c], first_ref[...], preferred_element_type=jnp.float32)
        real, imag = first[:, :RADIX], first[:, RADIX:]
        turn_real, turn_imag = twiddle_ref[0], twiddle_ref[1]
        lanes = slice((c % 2) * RADIX, (c % 2 + 1) * RADIX)
        mids[c // 2, :RADIX, lanes] = (real * turn_real - imag * turn_imag).astype(jnp.bfloat16)
        mids[c // 2, RADIX:, lanes] = (real * turn_imag + imag * turn_real).astype(jnp.bfloat16)
    for i in range(SUB // 2):
        spectrum = jnp.dot(second_ref[...], mids[i], preferred_element_type=jnp.float32)
        real, imag = spectrum[:OUT], spectrum[OUT:]
        power = real * real + imag * imag
        put(2 * i, power[:, :RADIX])
        put(2 * i + 1, power[:, RADIX:])


def local_kernel(
    groups, where, own, other, mask, first, twiddle, second, window, out, wide, sums, lhs, mids
):
    core, chip = where[0], where[1]
    ending = jnp.logical_and(chip == groups - 1, pl.program_id(0) >= groups // 2)
    tables = (first, twiddle, second)

    def block(n, _):
        for half in range(2):
            stage(wide.at[half], sums.at[half], own.at[n], half)
            stage(wide.at[2 + half], sums.at[2 + half], other.at[n], half)
        for c in range(SUB):
            for s in range(2):
                piece = (
                    wide.at[2 * s], wide.at[2 * s + 1], sums.at[2 * s], sums.at[2 * s + 1],
                    mask.at[n, s],
                )
                lhs[c, :, s * RADIX : (s + 1) * RADIX] = shape(c, piece, window)

        def put(c, power):
            out[n, c] = power

        pair_power(lhs, mids, tables, put)

        @pl.when(ending)
        def _():
            head = jnp.where(core == 1, 1, 3)
            tail = 4 - head
            wide[tail] = jnp.zeros_like(wide[tail])
            sums[tail] = jnp.zeros_like(sums[tail])
            piece = (wide.at[head], wide.at[tail], sums.at[head], sums.at[tail], mask.at[n, 2])
            for c in range(SUB):
                lhs[c, :, :RADIX] = shape(c, piece, window)
                lhs[c, :, RADIX:] = jnp.zeros((RADIX, RADIX), jnp.bfloat16)

            def add(c, power):
                out[n, c] = out[n, c] + power

            pair_power(lhs, mids, tables, add)

        return 0

    lax.fori_loop(0, own.shape[0], block, 0)


def cross_kernel(
    groups, sub, count, where, own, other, lower0, lower1, upper0, upper1, base, weight,
    first, twiddle, second, window, mirror, *rest,
):
    outs = rest[:count]
    load, held, wide, sums, lhs, mids, total, plain, turned, sems, held_sems = rest[count:]
    core = where[0]

    units = count * sub

    def find(u):
        index = u // sub
        group = where[2 + index]
        return index, group, group < groups // 2, u - index * sub

    def copy(source, slot, k):
        return pltpu.make_async_copy(source, load.at[slot, k], sems.at[slot, k])

    def fetch(u):
        slot = u & (DEPTH - 1)
        _, group, low, n = find(u)
        high = jnp.logical_not(low)
        edge = jnp.where(low, group, group - groups // 2) * sub
        inside = (2 * group + core) * sub
        for index, lo, hi, up, down in (
            (0, own, other, upper0, lower0),
            (1, other, own, upper1, lower1),
        ):
            here = core == index

            @pl.when(here)
            def _():
                copy(lo.at[inside + n, pl.ds(HALF, HALF)], slot, 0).start()
                copy(hi.at[inside + n, pl.ds(0, HALF)], slot, 1).start()

            @pl.when(jnp.logical_and(here, low))
            def _():
                copy(hi.at[inside + n, pl.ds(HALF, HALF)], slot, 2).start()
                copy(up.at[edge + n], slot, 3).start()

            @pl.when(jnp.logical_and(here, high))
            def _():
                copy(down.at[edge + n], slot, 2).start()
                copy(lo.at[inside + n, pl.ds(0, HALF)], slot, 3).start()

    held_copies = [
        pltpu.make_async_copy(base.at[pl.ds(where[2 + i] * sub, sub)], held.at[i], held_sems.at[i])
        for i in range(count)
    ]
    for u in range(min(DEPTH - 1, units)):
        fetch(u)
    for held_copy in held_copies:
        held_copy.start()
    lane = lax.broadcasted_iota(jnp.int32, (KBANDS, RADIX), 1)

    def unit(u, _):
        slot = u & (DEPTH - 1)
        index, group, low, n = find(u)

        @pl.when(u + DEPTH - 1 < units)
        def _():
            fetch(u + DEPTH - 1)

        for k in range(4):
            copy(upper0.at[0], slot, k).wait()

        row = group * sub + n
        for k in range(4):
            stage(wide.at[k], sums.at[k], load.at[slot, k], 0)
        masks = (1, jnp.where(low, 3, 4))
        for c in range(SUB):
            for s in range(2):
                piece = (
                    wide.at[2 * s], wide.at[2 * s + 1], sums.at[2 * s], sums.at[2 * s + 1],
                    weight.at[row, masks[s]],
                )
                lhs[c, :, s * RADIX : (s + 1) * RADIX] = shape(c, piece, window)

        for i in range(count):

            @pl.when(u == i * sub)
            def _():
                held_copies[i].wait()

        def put(c, power):
            total[c] = held[index, n, c] + power

        pair_power(lhs, mids, (first, twiddle, second), put)

        for c in range(SUB):
            rows = slice(c * KBANDS, (c + 1) * KBANDS)
            plain[rows, :] = total[c, :KBANDS]
            turned[rows, :] = jnp.where(
                lane == 0,
                total[c, KBANDS : 2 * KBANDS],
                total[c, KBANDS + 1 : 2 * KBANDS + 1],
            )
        plain[SUB * KBANDS :, :] = jnp.sum(weight[row, :4], axis=0)
        turned[SUB * KBANDS :, :] = jnp.zeros((SUB, RADIX), jnp.float32)
        reverse = jnp.dot(
            turned[...].astype(jnp.bfloat16), mirror[...], preferred_element_type=jnp.float32
        )
        packed = (plain[...] + reverse).astype(jnp.bfloat16)
        for i, out in enumerate(outs):

            @pl.when(index == i)
            def _():
                out[n] = packed

        return 0

    lax.fori_loop(0, units, unit, 0)


def finish_kernel(*refs):
    *pieces, scale, out, total = refs
    for n in range(out.shape[0] // SUB):
        value = pieces[0][n].astype(jnp.float32)
        for piece in pieces[1:]:
            value = value + piece[n].astype(jnp.float32)
        total[...] = value
        inverse = 1.0 / jnp.maximum(total[SUB * KBANDS :, :], 1.0)
        for j in range(KBANDS):
            value = total[pl.ds(j, SUB, stride=KBANDS), :]
            out[n * SUB : (n + 1) * SUB, j * RADIX : (j + 1) * RADIX] = (
                value * scale[j : j + 1, :] * inverse
            )


def whole(array):
    return pl.BlockSpec(array.shape, lambda *_: (0,) * array.ndim)


def per_device(samples, valid):
    first, twiddle, second, window, mirror, scale = make_tables()
    tables = (first, twiddle, second, window)
    channels = samples.shape[0]
    size = lax.axis_size("chan")
    chips = size // 2
    half = chips // 2
    place = lax.axis_index("chan")
    core, chip = place & 1, place >> 1
    sub = channels // (SUB * size)

    def send(value, perm):
        return lax.ppermute(value, "chan", perm)

    def tiled(value):
        return value.reshape(channels // SUB, SUB, RADIX, RADIX).transpose(0, 2, 1, 3)

    swap = [(i, i ^ 1) for i in range(size)]
    links = range(chips - 1)
    tiles = tiled(samples)
    groups = tiles.reshape(chips, 2, sub, RADIX, SUB, RADIX)
    edges = [
        lax.dynamic_slice(
            groups,
            (core * half, c, 0, core * HALF, 0, 0),
            (half, 1, sub, HALF, SUB, RADIX),
        ).reshape(half * sub, HALF, SUB, RADIX)
        for c in range(2)
    ]
    onward = [[(2 * z + 1, 2 * z + 2 + c) for z in links] for c in range(2)]
    back = [[(2 * z + 2, 2 * z + c) for z in links] for c in range(2)]
    lower = [send(edges[c], onward[c]) for c in range(2)]
    upper = [send(edges[c], back[c]) for c in range(2)]
    other = tiled(send(samples, swap))

    theirs = send(valid, swap)
    before = sum(send(valid, onward[c]) for c in range(2))

    def spread(mask):
        count = mask.shape[1]
        mask = mask.astype(jnp.float32).reshape(chips, 2, sub, SUB, count)
        mask = lax.dynamic_index_in_dim(mask, core, 1, False).reshape(chips * sub, SUB, count)
        shape = (chips * sub, count, SUB, RADIX)
        return jnp.broadcast_to(mask.transpose(0, 2, 1)[..., None], shape)

    lo = jnp.where(core == 0, valid, theirs)
    hi = jnp.where(core == 0, theirs, valid)
    step = 2 if sub % 2 == 0 else 1
    tile = (step, RADIX, SUB, RADIX)
    stripe = STEP * SUB
    wide_shape = pltpu.VMEM((4, stripe, RADIX), jnp.float32)
    sums_shape = pltpu.VMEM((4, SUB, RADIX), jnp.float32)
    lhs_shape = pltpu.VMEM((SUB, RADIX, 2 * RADIX), jnp.bfloat16)
    mids_shape = pltpu.VMEM((SUB // 2, 2 * RADIX, 2 * RADIX), jnp.bfloat16)
    local_grid = (chips, sub // step)

    def dense(g, i, w):
        return (g * (sub // step) + i, 0, 0, 0)

    def mine(g, i, w):
        return ((2 * g + w[0]) * (sub // step) + i, 0, 0, 0)

    local_mask = spread(jnp.concatenate([valid[:, :1], theirs[:, :1], hi[:, 1:]], axis=1))
    where = jnp.stack([core, chip]).astype(jnp.int32)
    partial = pl.pallas_call(
        functools.partial(local_kernel, chips),
        grid_spec=pltpu.PrefetchScalarGridSpec(
            num_scalar_prefetch=1,
            grid=local_grid,
            in_specs=[
                pl.BlockSpec(tile, mine),
                pl.BlockSpec(tile, mine),
                pl.BlockSpec((step, 3, SUB, RADIX), dense),
                *[whole(t) for t in tables],
            ],
            out_specs=pl.BlockSpec((step, SUB, OUT, RADIX), dense),
            scratch_shapes=[wide_shape, sums_shape, lhs_shape, mids_shape],
        ),
        out_shape=jax.ShapeDtypeStruct((chips * sub, SUB, OUT, RADIX), jnp.float32),
        name="local_segments",
    )(where, tiles, other, local_mask, *tables)

    before, _ = lax.optimization_barrier((before, partial))
    weight = spread(jnp.concatenate([lo, hi, before[:, 1:]], axis=1))

    anywhere = pl.BlockSpec(memory_space=pl.ANY)

    def cross(targets):
        count = len(targets)
        return pl.pallas_call(
            functools.partial(cross_kernel, chips, sub, count),
            grid_spec=pltpu.PrefetchScalarGridSpec(
                num_scalar_prefetch=1,
                grid=(1,),
                in_specs=[
                    *[anywhere] * 7,
                    whole(weight),
                    *[whole(t) for t in tables],
                    whole(mirror),
                ],
                out_specs=[pl.BlockSpec((sub, ROWS, RADIX), lambda i, w: (0, 0, 0))] * count,
                scratch_shapes=[
                    pltpu.VMEM((DEPTH, 4, HALF, SUB, RADIX), jnp.bfloat16),
                    pltpu.VMEM((count, sub, SUB, OUT, RADIX), jnp.float32),
                    wide_shape,
                    sums_shape,
                    lhs_shape,
                    mids_shape,
                    pltpu.VMEM((SUB, OUT, RADIX), jnp.float32),
                    pltpu.VMEM((ROWS, RADIX), jnp.float32),
                    pltpu.VMEM((ROWS, RADIX), jnp.float32),
                    pltpu.SemaphoreType.DMA((DEPTH, 4)),
                    pltpu.SemaphoreType.DMA((count,)),
                ],
            ),
            out_shape=[jax.ShapeDtypeStruct((sub, ROWS, RADIX), jnp.bfloat16)] * count,
        )(
            jnp.stack([core, chip, *targets]).astype(jnp.int32),
            tiles, other, *lower, *upper, partial, weight, *tables, mirror,
        )

    shifts = sorted(range(1, chips), key=lambda r: (-min(r, chips - r), r)) + [0]
    targets = [jnp.where(chip + r >= chips, chip + r - chips, chip + r) for r in shifts]
    early = cross(targets[:half])
    rest, _ = lax.optimization_barrier((jnp.stack(targets[half:]), early[-1]))
    late = cross([rest[i] for i in range(chips - half)])
    pieces = [*early, *late]
    for k, shift in enumerate(shifts[:-1]):
        around = [(i, (i + 2 * shift) % size) for i in range(size)]
        pieces[k] = send(pieces[k], around)

    return pl.pallas_call(
        finish_kernel,
        in_specs=[pl.BlockSpec(memory_space=pltpu.VMEM)] * (chips + 1),
        out_specs=pl.BlockSpec(memory_space=pltpu.VMEM),
        out_shape=jax.ShapeDtypeStruct((sub * SUB, KBANDS * RADIX), jnp.float32),
        scratch_shapes=[pltpu.VMEM((ROWS, RADIX), jnp.float32)],
        name="finish",
    )(*pieces, scale)


def solution(mesh):
    return jax.shard_map(
        per_device,
        mesh=mesh,
        in_specs=(P("tm", "chan"), P("tm", "chan")),
        out_specs=P(("tm", "chan"), None),
        check_vma=False,
    )
```
